32 devices in a mesh: dp: 4 (over z), fsdp: 8 (over y, x, core).
Axes of the slice: x: 2, y: 2, z: 4, core: 2. Of those that a mesh axis runs over, the one named last changes fastest.
Arguments:
- x_in: bfloat16 [192, 256, 512], P(('dp', 'fsdp'))
- positions: int32 [192, 256], P(('dp', 'fsdp'))
- segments: int32 [192, 256], P(('dp', 'fsdp'))
- rel_bias: float32 [32, 6], replicated
- gain_attn: float32 [512], replicated
- gain_mlp: float32 [512], replicated
- w_q: bfloat16 [512, 384], P('fsdp')
- w_k: bfloat16 [512, 384], P('fsdp')
- w_v: bfloat16 [512, 384], P('fsdp')
- w_o: bfloat16 [384, 512], P('fsdp')
- w_i0: bfloat16 [512, 1024], P('fsdp')
- w_i1: bfloat16 [512, 1024], P('fsdp')
- w_f: bfloat16 [1024, 512], P('fsdp')
- grad_out: bfloat16 [192, 256, 512], P(('dp', 'fsdp'))
Outputs:
- output 1: bfloat16 [192, 256, 512], P(('dp', 'fsdp'))
- output 2: float32 [32, 6], replicated
- output 3: float32 [512], replicated
- output 4: float32 [512], replicated
- output 5: bfloat16 [512, 384], P('fsdp')
- output 6: bfloat16 [512, 384], P('fsdp')
- output 7: bfloat16 [512, 384], P('fsdp')
- output 8: bfloat16 [384, 512], P('fsdp')
- output 9: bfloat16 [512, 1024], P('fsdp')
- output 10: bfloat16 [512, 1024], P('fsdp')
- output 11: bfloat16 [1024, 512], P('fsdp')
All inputs are finite; a program needn't handle non-finite values.
Results may differ from the reference program's by a relative error of at most 0.0185089.
Values are sent between devices in bfloat16 or wider.
A program may use at most 1 GiB of HBM per device.

```python
import jax
import jax.numpy as jnp
from jax import lax

BATCH_ROWS = 192
SEQ_LEN = 256
D_MODEL = 512
HEADS = 6
HEAD_DIM = 64
FF_DIM = 1024
REL_CLASSES = 32
HALF_CLASSES = REL_CLASSES // 2
EXACT_RANGE = HALF_CLASSES // 2
THRESHOLDS = (12, 16, 23, 32, 46, 64, 91)
EPSILON = 1e-6
NEG_BIG = -1e9


def draw_segments(key):
    margin = SEQ_LEN // 8
    cuts = jax.random.randint(key, (BATCH_ROWS, 2), margin, SEQ_LEN - margin + 1)
    first_cut = jnp.min(cuts, axis=1, keepdims=True)
    second_cut = jnp.max(cuts, axis=1, keepdims=True)
    index = jnp.arange(SEQ_LEN, dtype=jnp.int32)[None, :]
    segments = (index >= first_cut).astype(jnp.int32) + (index >= second_cut).astype(jnp.int32)
    start = jnp.where(segments == 0, 0, jnp.where(segments == 1, first_cut, second_cut))
    positions = (index - start).astype(jnp.int32)
    return positions, segments


def setup_inputs(seed: int = 0) -> dict:
    keys = jax.random.split(jax.random.key(seed), 14)
    width = HEADS * HEAD_DIM
    act_shape = (BATCH_ROWS, SEQ_LEN, D_MODEL)
    score_scale = D_MODEL ** -0.5 * (2.0 / HEAD_DIM) ** 0.25

    def draw_normal(key, shape, scale):
        return jax.random.normal(key, shape, jnp.float32) * scale

    x_in = draw_normal(keys[0], act_shape, 1.0).astype(jnp.bfloat16)
    positions, segments = draw_segments(keys[1])
    rel_bias = draw_normal(keys[2], (REL_CLASSES, HEADS), 1.0)
    gain_attn = 1.0 + draw_normal(keys[3], (D_MODEL,), 0.4)
    gain_mlp = 1.0 + draw_normal(keys[4], (D_MODEL,), 0.4)
    w_q = draw_normal(keys[5], (D_MODEL, width), score_scale).astype(jnp.bfloat16)
    w_k = draw_normal(keys[6], (D_MODEL, width), score_scale).astype(jnp.bfloat16)
    w_v = draw_normal(keys[7], (D_MODEL, width), D_MODEL ** -0.5).astype(jnp.bfloat16)
    w_o = draw_normal(keys[8], (width, D_MODEL), 2.0 * width ** -0.5).astype(jnp.bfloat16)
    w_i0 = draw_normal(keys[9], (D_MODEL, FF_DIM), D_MODEL ** -0.5).astype(jnp.bfloat16)
    w_i1 = draw_normal(keys[10], (D_MODEL, FF_DIM), D_MODEL ** -0.5).astype(jnp.bfloat16)
    w_f = draw_normal(keys[11], (FF_DIM, D_MODEL), 2.0 * FF_DIM ** -0.5).astype(jnp.bfloat16)
    grad_out = draw_normal(keys[12], act_shape, 1.0).astype(jnp.bfloat16)
    return {'x_in': x_in, 'positions': positions, 'segments': segments, 'rel_bias': rel_bias,
            'gain_attn': gain_attn, 'gain_mlp': gain_mlp, 'w_q': w_q, 'w_k': w_k, 'w_v': w_v,
            'w_o': w_o, 'w_i0': w_i0, 'w_i1': w_i1, 'w_f': w_f, 'grad_out': grad_out}


def mat(left, right):
    return jnp.dot(left.astype(jnp.float32), right.astype(jnp.float32))


def rms_norm(values, gain):
    inv_rms = lax.rsqrt(jnp.mean(values * values, axis=-1, keepdims=True) + EPSILON)
    return (values * inv_rms * gain).astype(jnp.bfloat16)


def rel_class(pos_row):
    offset = pos_row[None, :] - pos_row[:, None]
    distance = jnp.abs(offset)
    magnitude = jnp.minimum(distance, EXACT_RANGE)
    for bound in THRESHOLDS:
        magnitude = magnitude + (distance >= bound).astype(jnp.int32)
    return magnitude + HALF_CLASSES * (offset > 0).astype(jnp.int32)


def attend_row(q_row, k_row, v_row, pos_row, seg_row, rel_bias):
    scores = jnp.einsum('qhd,khd->hqk', q_row.astype(jnp.float32), k_row.astype(jnp.float32))
    bias = jnp.transpose(rel_bias[rel_class(pos_row)], (2, 0, 1))
    same_seg = seg_row[:, None] == seg_row[None, :]
    scores = scores + bias + jnp.where(same_seg, 0.0, NEG_BIG)
    attn_prob = jax.nn.softmax(scores, axis=-1)
    context = jnp.einsum('hqk,khd->qhd', attn_prob.astype(jnp.bfloat16).astype(jnp.float32), v_row.astype(jnp.float32))
    return context.astype(jnp.bfloat16)


def layer(x_in, positions, segments, param_set):
    rel_bias, gain_attn, gain_mlp, w_q, w_k, w_v, w_o, w_i0, w_i1, w_f = param_set
    rows, seq_len, width = x_in.shape
    heads = rel_bias.shape[1]
    x_float = x_in.astype(jnp.float32).reshape(rows * seq_len, width)
    normed = rms_norm(x_float, gain_attn)
    q_all = mat(normed, w_q).astype(jnp.bfloat16).reshape(rows, seq_len, heads, -1)
    k_all = mat(normed, w_k).astype(jnp.bfloat16).reshape(rows, seq_len, heads, -1)
    v_all = mat(normed, w_v).astype(jnp.bfloat16).reshape(rows, seq_len, heads, -1)
    row_attend = jax.checkpoint(lambda row_args: attend_row(row_args[0], row_args[1], row_args[2], row_args[3], row_args[4], rel_bias))
    context = lax.map(row_attend, (q_all, k_all, v_all, positions, segments))
    context = context.reshape(rows * seq_len, -1)
    hidden = (x_float + mat(context, w_o)).astype(jnp.bfloat16)
    h_float = hidden.astype(jnp.float32)
    mlp_in = rms_norm(h_float, gain_mlp)
    hidden_act = (jax.nn.silu(mat(mlp_in, w_i0)) * mat(mlp_in, w_i1)).astype(jnp.bfloat16)
    y_out = (h_float + mat(hidden_act, w_f)).astype(jnp.bfloat16)
    return y_out.reshape(rows, seq_len, width)


def reference(x_in, positions, segments, rel_bias, gain_attn, gain_mlp, w_q, w_k, w_v, w_o, w_i0, w_i1, w_f, grad_out):
    param_set = (rel_bias, gain_attn, gain_mlp, w_q, w_k, w_v, w_o, w_i0, w_i1, w_f)
    y_out, pull_back = jax.vjp(lambda params_in: layer(x_in, positions, segments, params_in), param_set)
    grads = pull_back(grad_out)[0]
    return (y_out, grads[0], grads[1], grads[2], grads[3], grads[4], grads[5], grads[6], grads[7], grads[8], grads[9])
```

```python
import functools

import jax
import jax.numpy as jnp
from jax import lax
from jax.experimental import pallas as pl
from jax.experimental.pallas import tpu as pltpu
from jax.sharding import PartitionSpec as P

EPSILON = 1e-6
NEG_BIG = -1e9
THRESHOLDS = (12, 16, 23, 32, 46, 64, 91)
ROW_AXES = ('dp', 'fsdp')
ROWS, SEQ, DM, HEADS, HD, FF = 6, 256, 512, 6, 64, 1024
TOK = ROWS * SEQ
AW = HEADS * HD
F32, BF16 = jnp.float32, jnp.bfloat16


def mm(a, b):
    return lax.dot_general(a, b, (((1,), (0,)), ((), ())), preferred_element_type=F32)


def mm_nt(a, b):
    return lax.dot_general(a, b, (((1,), (1,)), ((), ())), preferred_element_type=F32)


def mm_tn(a, b):
    return lax.dot_general(a, b, (((0,), (0,)), ((), ())), preferred_element_type=F32)


def split3(v):
    hi = v.astype(BF16)
    rest = v - hi.astype(F32)
    mid = rest.astype(BF16)
    lo = (rest - mid.astype(F32)).astype(BF16)
    return hi, mid, lo


def tok_slice(r):
    return pl.ds(pl.multiple_of(r * SEQ, SEQ), SEQ)


def rel_class(diff):
    m = jnp.abs(diff)
    e = jnp.minimum(m, 8.0)
    for bound in THRESHOLDS:
        e = e + jnp.where(m >= bound, 1.0, 0.0)
    return e + jnp.where(diff > 0, 16.0, 0.0)


def setup_small(relb_ref, ga_ref, gm_ref, tab_s, pad_s, ga_s, gm_s):
    pad_s[...] = jnp.zeros_like(pad_s)
    pad_s[0:32, 0:HEADS] = relb_ref[...]
    t = pad_s[...].T[0:8, :]
    lane = lax.broadcasted_iota(jnp.int32, t.shape, 1)
    tab_s[...] = jnp.where(lane < 32, t, pltpu.roll(t, 32, 1) + NEG_BIG)
    ga_s[...] = jnp.broadcast_to(ga_ref[...], (128, DM)).T
    gm_s[...] = jnp.broadcast_to(gm_ref[...], (128, DM)).T


def wide(col128):
    return jnp.concatenate([col128, col128], axis=1)


def attn_fwd_row(r, x_ref, pos_ref, seg_ref, tab_s, ga_s, wqkvt_s, xt_s, qkv_s, p_s, ctx_s):
    tok = tok_slice(r)
    xt = x_ref[pl.ds(pl.multiple_of(r * SEQ, SEQ), SEQ), :].T
    xt_s[:, tok] = xt
    xf = xt.astype(F32)
    inv = lax.rsqrt(jnp.mean(xf * xf, axis=0, keepdims=True) + EPSILON)
    at = (xf * inv * wide(ga_s[...])).astype(BF16)
    qkv_s[:, tok] = mm(wqkvt_s[...], at).astype(BF16)
    code = (seg_ref[r] * 1024 + pos_ref[r]).astype(F32)
    code = jnp.broadcast_to(code, (SEQ, SEQ))
    diff = code.T - code
    idx = (rel_class(diff) + jnp.where(jnp.abs(diff) >= 512.0, 32.0, 0.0)).astype(jnp.int32)
    for h in range(HEADS):
        qt = qkv_s[h * HD:(h + 1) * HD, tok]
        kt = qkv_s[AW + h * HD:AW + (h + 1) * HD, tok]
        vt = qkv_s[2 * AW + h * HD:2 * AW + (h + 1) * HD, tok]
        table = jnp.broadcast_to(tab_s[h:h + 1, :], (SEQ, 128))
        bias = jnp.concatenate([jnp.take_along_axis(table, idx[:, 0:128], axis=1),
                                jnp.take_along_axis(table, idx[:, 128:256], axis=1)], axis=1)
        s = mm_tn(kt, qt) + bias
        p = jnp.exp(s - jnp.max(s, axis=0, keepdims=True))
        p = p * (1.0 / jnp.sum(p, axis=0, keepdims=True))
        p_s[h, r] = p
        ctx_s[h * HD:(h + 1) * HD, tok] = mm(vt, p.astype(BF16)).astype(BF16)


def mlp_row(r, go_ref, y_ref, gm_s, wot_s, wit_s, wft_s, wi_s, wf_s, xt_s, ctx_s, got_s, ut_s, zt_s, dgu_s, dh_s, dgm_s):
    tok = tok_slice(r)
    rows = pl.ds(pl.multiple_of(r * SEQ, SEQ), SEQ)
    ht = (xt_s[:, tok].astype(F32) + mm(wot_s[...], ctx_s[:, tok])).astype(BF16)
    hf = ht.astype(F32)
    inv = lax.rsqrt(jnp.mean(hf * hf, axis=0, keepdims=True) + EPSILON)
    gm = wide(gm_s[...])
    ut = (hf * inv * gm).astype(BF16)
    ut_s[:, tok] = ut
    got = go_ref[rows, :].T
    got_s[:, tok] = got
    step = 256
    for f in range(0, FF, step):
        gate = mm(wit_s[f:f + step, :], ut)
        up = mm(wit_s[FF + f:FF + f + step, :], ut)
        dz = mm(wf_s[f:f + step, :], got).astype(BF16).astype(F32)
        sg = 1.0 / (1.0 + jnp.exp(-gate))
        silu = gate * sg
        zt_s[f:f + step, tok] = (silu * up).astype(BF16)
        dgu_s[f:f + step, tok] = (dz * up * (sg * (1.0 + gate * (1.0 - sg)))).astype(BF16)
        dgu_s[FF + f:FF + f + step, tok] = (dz * silu).astype(BF16)
    yt = (hf + mm(wft_s[...], zt_s[:, tok])).astype(BF16)
    y_ref[rows, :] = yt.T
    du = mm(wi_s[...], dgu_s[:, tok]).astype(BF16).astype(F32)
    hn = hf * inv
    dg = du * hn
    dgm_s[...] += dg[:, 0:128] + dg[:, 128:256]
    dug = du * gm
    dhn = inv * (dug - hn * jnp.mean(dug * hn, axis=0, keepdims=True))
    dh_s[:, tok] = (got.astype(F32) + dhn).astype(BF16)


def attn_bwd_row(r, pos_ref, ga_s, wqkv_s, wo_s, xt_s, at_s, qkv_s, p_s, dh_s, dqkv_s, dacc_s, dga_s):
    tok = tok_slice(r)
    dct = mm(wo_s[...], dh_s[:, tok]).astype(BF16)
    pos = pos_ref[r]
    onehot = jnp.where(lax.broadcasted_iota(jnp.int32, (SEQ, SEQ), 0) == pos, 1.0, 0.0).astype(BF16)
    for h in range(HEADS):
        qt = qkv_s[h * HD:(h + 1) * HD, tok]
        kt = qkv_s[AW + h * HD:AW + (h + 1) * HD, tok]
        vt = qkv_s[2 * AW + h * HD:2 * AW + (h + 1) * HD, tok]
        dc = dct[h * HD:(h + 1) * HD, :]
        p = p_s[h, r]
        dp = mm_tn(vt, dc)
        ds = p * (dp - jnp.sum(dp * p, axis=0, keepdims=True))
        dqkv_s[2 * AW + h * HD:2 * AW + (h + 1) * HD, tok] = mm_nt(dc, p.astype(BF16)).astype(BF16)
        hi, mid, lo = split3(ds)
        dqkv_s[h * HD:(h + 1) * HD, tok] = mm(kt, hi).astype(BF16)
        dqkv_s[AW + h * HD:AW + (h + 1) * HD, tok] = mm_nt(qt, hi).astype(BF16)
        t = mm(onehot, hi) + mm(onehot, mid) + mm(onehot, lo)
        hi, mid, lo = split3(t)
        dacc_s[h] += mm_nt(hi, onehot) + mm_nt(mid, onehot) + mm_nt(lo, onehot)
    dn = mm(wqkv_s[...], dqkv_s[0:3 * AW, tok]).astype(BF16).astype(F32)
    xf = xt_s[:, tok].astype(F32)
    inv = lax.rsqrt(jnp.mean(xf * xf, axis=0, keepdims=True) + EPSILON)
    xn = xf * inv
    at_s[:, tok] = (xn * wide(ga_s[...])).astype(BF16)
    dg = dn * xn
    dga_s[...] += dg[:, 0:128] + dg[:, 128:256]


def bias_sums(dacc_s, db_s):
    db_s[...] = jnp.zeros_like(db_s)
    diff = (lax.broadcasted_iota(jnp.int32, (SEQ, SEQ), 0) - lax.broadcasted_iota(jnp.int32, (SEQ, SEQ), 1)).astype(F32)
    cls = rel_class(diff)

    def body(c, carry):
        hit = cls == c.astype(F32)
        for h in range(HEADS):
            db_s[pl.ds(c * 8 + h, 1), :] = jnp.sum(jnp.where(hit, dacc_s[h], 0.0), axis=0, keepdims=True)
        return carry
    lax.fori_loop(0, 32, body, 0)


def loop(n, fn):
    def body(i, carry):
        fn(i)
        return carry
    lax.fori_loop(0, n, body, 0)


MESH = pl.DeviceIdType.MESH
SHARD = ((128, 512), (64, 2048), (48, 512), (64, 1152))
WF, WI, WO, WQKV = 0, 1, 2, 3
NSEM = 16


def remote(src, dst, send, recv, i, dev):
    return pltpu.make_async_remote_copy(src_ref=src, dst_ref=dst, send_sem=send.at[i], recv_sem=recv.at[i],
                                        device_id=dev, device_id_type=MESH)


class Place:
    def __init__(self):
        self.f = lax.axis_index('fsdp')
        self.z = lax.axis_index('dp')
        self.c = lax.rem(self.f, 2)
        self.k = self.f // 2
        self.x = lax.rem(self.k, 2)
        self.y = self.k // 2
        self.kx = self.k + 1 - 2 * self.x
        self.ky = self.k + 2 - 4 * self.y
        self.kd = 3 - self.k
        self.sib = {'fsdp': self.f + 1 - 2 * self.c}
        self.nx = {'fsdp': 2 * self.kx + self.c}
        self.ny = {'fsdp': 2 * self.ky + self.c}
        self.nd = {'fsdp': 2 * self.kd + self.c}
        self.up = [lax.rem(self.z + j, 4) for j in (1, 2, 3)]
        self.nz = [{'dp': u} for u in self.up]


class Gather:
    def __init__(self, at, parts, fulls, own, send, recv):
        self.at, self.parts, self.fulls, self.own, self.send, self.recv = at, parts, fulls, own, send, recv

    def view(self, w, f):
        full, col = self.fulls[w]
        rows, cols = self.parts[w].shape
        return full.at[pl.ds(pl.multiple_of(f * rows, rows), rows), pl.ds(col, cols)]

    def load(self, w):
        return pltpu.make_async_copy(self.parts[w], self.view(w, self.at.f), self.own.at[w])

    def direct(self, w, j):
        at = self.at
        v = self.view(w, at.f)
        return remote(v, v, self.send, self.recv, w * 7 + j, (at.nx, at.ny, at.nd, at.sib)[j])

    def forward(self, w, j):
        at = self.at
        v = self.view(w, 2 * (at.kx, at.ky, at.kd)[j] + at.c)
        return remote(v, v, self.send, self.recv, w * 7 + 4 + j, at.sib)

    def begin(self, ws):
        for w in ws:
            self.load(w).wait()
            for j in (2, 0, 1, 3):
                self.direct(w, j).start()

    def relay(self, ws):
        for w in ws:
            for j in (0, 1, 2):
                self.direct(w, j).wait_recv()
                self.forward(w, j).start()

    def finish(self, ws):
        for w in ws:
            self.direct(w, 3).wait_recv()
            for j in (0, 1, 2):
                self.forward(w, j).wait_recv()

    def drain(self):
        for w in range(len(self.parts)):
            for j in range(4):
                self.direct(w, j).wait_send()
            for j in range(3):
                self.forward(w, j).wait_send()


class Reduce:
    def __init__(self, a, at, acc, rd, r1, r2, rz, out, send, recv):
        self.a, self.at, self.acc, self.rd, self.r1, self.r2, self.rz, self.out = a, at, acc, rd, r1, r2, rz, out
        self.send, self.recv = send, recv
        self.rows, self.cols = SHARD[a]
        self.half = self.rows // 2

    def part(self, k, c, h=None):
        n = self.rows if h is None else self.half
        off = (2 * k + c) * self.rows + (0 if h is None else h * self.half)
        return self.acc.at[pl.ds(pl.multiple_of(off, 8), n), :]

    def copy(self, src, dst, i, dev):
        return remote(src, dst, self.send, self.recv, self.a * NSEM + i, dev)

    def d_copy(self, i):
        at = self.at
        k = (at.kd, at.kx, at.ky, at.k)[i]
        return self.copy(self.part(k, 1 - at.c), self.rd.at[i], i, at.sib)

    def xy1_copy(self, i):
        at = self.at
        k, h, dev = ((at.kx, 0, at.nx), (at.kd, 0, at.nx), (at.ky, 1, at.ny), (at.kd, 1, at.ny))[i]
        return self.copy(self.part(k, at.c, h), self.r1.at[i], 4 + i, dev)

    def xy2_copy(self, i):
        at = self.at
        k, h, dev = ((at.ky, 0, at.ny), (at.kx, 1, at.nx))[i]
        return self.copy(self.part(k, at.c, h), self.r2.at[i], 8 + i, dev)

    def quarter(self, z, base):
        if self.rows == 48:
            return pl.ds(base, self.rows), pl.ds(pl.multiple_of(z * 128, 128), 128)
        n = self.rows // 4
        return pl.ds(pl.multiple_of(base + z * n, 16), n), slice(None)

    def z1_copy(self, j):
        at = self.at
        rows, cols = self.quarter(at.up[j], pl.multiple_of(at.f * self.rows, 16))
        return self.copy(self.acc.at[rows, cols], self.rz.at[j], 10 + j, at.nz[j])

    def z2_copy(self, j):
        at = self.at
        rows, cols = self.quarter(at.z, 0)
        v = self.out.at[rows, cols]
        return self.copy(v, v, 13 + j, at.nz[j])

    def d_send(self):
        for i in range(4):
            self.d_copy(i).start()

    def add(self, view, buf):
        view[...] = view[...] + buf[...]

    def xy1(self):
        at = self.at
        for i, k in enumerate((at.kd, at.kx, at.ky, at.k)):
            self.d_copy(i).wait_recv()
            self.add(self.part(k, at.c), self.rd.at[i])
        for i in (0, 2, 1, 3):
            self.xy1_copy(i).start()

    def xy2(self):
        at = self.at
        for i, (k, h) in ((1, (at.ky, 0)), (3, (at.kx, 1)), (0, (at.k, 0)), (2, (at.k, 1))):
            self.xy1_copy(i).wait_recv()
            self.add(self.part(k, at.c, h), self.r1.at[i])
            if i == 1:
                self.xy2_copy(0).start()
            if i == 3:
                self.xy2_copy(1).start()

    def z1(self):
        at = self.at
        for i in range(2):
            self.xy2_copy(i).wait_recv()
            self.add(self.part(at.k, at.c, i), self.r2.at[i])
        for j in (1, 0, 2):
            self.z1_copy(j).start()

    def z2(self):
        at = self.at
        rows, cols = self.quarter(at.z, pl.multiple_of(at.f * self.rows, 16))
        total = self.acc[rows, cols]
        for j in range(3):
            self.z1_copy(j).wait_recv()
            total = total + self.rz[j]
        rows, cols = self.quarter(at.z, 0)
        self.out[rows, cols] = total.astype(BF16)
        for j in (1, 0, 2):
            self.z2_copy(j).start()

    def finish(self):
        for j in range(3):
            self.z2_copy(j).wait_recv()

    def drain(self):
        for i in range(4):
            self.d_copy(i).wait_send()
            self.xy1_copy(i).wait_send()
        for i in range(2):
            self.xy2_copy(i).wait_send()
        for i in range(3):
            self.z1_copy(i).wait_send()
            self.z2_copy(i).wait_send()


class Small:
    def __init__(self, at, sm, smr, smz, send, recv):
        self.at, self.sm, self.smr, self.smz, self.send, self.recv = at, sm, smr, smz, send, recv
        self.base = 4 * NSEM

    def step(self, i):
        at = self.at
        return remote(self.sm.at[i], self.smr.at[i], self.send, self.recv, self.base + i, (at.sib, at.nx, at.ny)[i])

    def zcopy(self, j):
        v = self.smz.at[self.at.z]
        return remote(v, v, self.send, self.recv, self.base + 3 + j, self.at.nz[j])

    def advance(self, i):
        if i > 0:
            self.step(i - 1).wait_recv()
            total = self.sm[i - 1] + self.smr[i - 1]
            if i < 3:
                self.sm[i] = total
            else:
                self.smz[self.at.z] = total
        if i < 3:
            self.step(i).start()
        else:
            for j in range(3):
                self.zcopy(j).start()

    def finish(self):
        for j in range(3):
            self.zcopy(j).wait_recv()
        return (self.smz[0] + self.smz[1]) + (self.smz[2] + self.smz[3])

    def drain(self):
        for i in range(3):
            self.step(i).wait_send()
            self.zcopy(i).wait_send()


def layer_kernel(x_hbm, pos_ref, seg_ref, relb_ref, ga_ref, gm_ref, wq_ref, wk_ref, wv_ref, wo_ref, wi0_ref, wi1_ref, wf_ref, go_hbm,
                 y_hbm, small_ref, dq_ref, dk_ref, dv_ref, do_ref, di0_ref, di1_ref, df_ref,
                 tab_s, pad_s, ga_s, gm_s, wqkv_s, wo_s, wi_s, wf_s, wqkvt_s, wot_s, wit_s, wft_s, xt_s, qkv_s, p_s, ctx_s,
                 got_s, ut_s, zt_s, dgu_s, dh_s, dacc_s, dga_s, dgm_s, io_s,
                 gf_s, gi_s, go_s, gq_s, rd_f, rd_i, rd_o, rd_q, r1_f, r1_i, r1_o, r1_q, r2_f, r2_i, r2_o, r2_q,
                 rz_f, rz_i, rz_o, rz_q, out_f, out_i, out_o, out_q, sm_s, smr_s, smz_s,
                 io_sem, out_sem, ag_own, ag_send, ag_recv, rs_send, rs_recv):
    at = Place()
    barrier = pltpu.get_barrier_semaphore()
    peers = [at.sib, at.nx, at.ny, at.nd] + at.nz
    for dev in peers:
        pl.semaphore_signal(barrier, inc=1, device_id=dev, device_id_type=MESH)

    def rows_of(r):
        return pl.ds(pl.multiple_of(r * SEQ, SEQ), SEQ)

    def x_copy(r):
        return pltpu.make_async_copy(x_hbm.at[rows_of(r), :], io_s.at[rows_of(r), :], io_sem.at[0, r])

    def go_copy(r):
        return pltpu.make_async_copy(go_hbm.at[rows_of(r), :], io_s.at[rows_of(r), :], io_sem.at[1, r])

    def y_copy(r):
        return pltpu.make_async_copy(io_s.at[rows_of(r), :], y_hbm.at[rows_of(r), :], io_sem.at[2, r])

    gather = Gather(at, (wq_ref, wk_ref, wv_ref, wo_ref, wi0_ref, wi1_ref, wf_ref),
                    ((wqkv_s, 0), (wqkv_s, AW), (wqkv_s, 2 * AW), (wo_s, 0), (wi_s, 0), (wi_s, FF), (wf_s, 0)), ag_own, ag_send, ag_recv)
    for w in range(7):
        gather.load(w).start()
    for r in range(ROWS):
        x_copy(r).start()
    pl.semaphore_wait(barrier, len(peers))
    first, rest = (0, 1, 2), (3, 4, 5, 6)
    gather.begin(first)
    gather.begin(rest)
    setup_small(relb_ref, ga_ref, gm_ref, tab_s, pad_s, ga_s, gm_s)
    dgm_s[...] = jnp.zeros_like(dgm_s)
    dga_s[...] = jnp.zeros_like(dga_s)
    dacc_s[...] = jnp.zeros_like(dacc_s)
    gather.relay(first)
    gather.finish(first)
    wqkvt_s[...] = wqkv_s[...].T

    def fwd(r):
        x_copy(r).wait()
        attn_fwd_row(r, io_s, pos_ref, seg_ref, tab_s, ga_s, wqkvt_s, xt_s, qkv_s, p_s, ctx_s)
        go_copy(r).start()

        @pl.when(r == 4)
        def _():
            gather.relay(rest)
    loop(ROWS, fwd)
    gather.finish(rest)
    wot_s[...] = wo_s[...].T
    wft_s[...] = wf_s[...].T
    wit_s[...] = wi_s[...].T

    def mlp(r):
        go_copy(r).wait()
        mlp_row(r, io_s, io_s, gm_s, wot_s, wit_s, wft_s, wi_s, wf_s, xt_s, ctx_s, got_s, ut_s, zt_s, dgu_s, dh_s, dgm_s)
        y_copy(r).start()
    loop(ROWS, mlp)

    red = [Reduce(WF, at, gf_s, rd_f, r1_f, r2_f, rz_f, out_f, rs_send, rs_recv),
           Reduce(WI, at, gi_s, rd_i, r1_i, r2_i, rz_i, out_i, rs_send, rs_recv),
           Reduce(WO, at, go_s, rd_o, r1_o, r2_o, rz_o, out_o, rs_send, rs_recv),
           Reduce(WQKV, at, gq_s, rd_q, r1_q, r2_q, rz_q, out_q, rs_send, rs_recv)]
    small = Small(at, sm_s, smr_s, smz_s, rs_send, rs_recv)

    def dwf(c):
        part = pl.ds(pl.multiple_of(c * 256, 256), 256)
        gf_s[:, part] = mm_nt(zt_s[...], got_s[part, :])
    loop(2, dwf)
    red[WF].d_send()

    def dwi(c):
        part = pl.ds(pl.multiple_of(c * 256, 256), 256)
        gi_s[:, part] = mm_nt(ut_s[...], dgu_s[part, :])
    loop(8, dwi)
    red[WI].d_send()
    red[WF].xy1()

    def dwo(c):
        part = pl.ds(pl.multiple_of(c * 256, 256), 256)
        go_s[:, part] = mm_nt(ctx_s[...], dh_s[part, :])
    loop(2, dwo)
    red[WO].d_send()
    red[WI].xy1()

    def bwd(r):
        attn_bwd_row(r, pos_ref, ga_s, wqkv_s, wo_s, xt_s, ut_s, qkv_s, p_s, dh_s, dgu_s, dacc_s, dga_s)

        @pl.when(r == 0)
        def _():
            red[WO].xy1()
            red[WF].xy2()

        @pl.when(r == 1)
        def _():
            red[WF].z1()

        @pl.when(r == 2)
        def _():
            red[WI].xy2()
            red[WO].xy2()

        @pl.when(r == 3)
        def _():
            red[WF].z2()
            red[WI].z1()

        @pl.when(r == 4)
        def _():
            red[WO].z1()
    loop(ROWS, bwd)

    def dwqkv(c):
        part = pl.ds(pl.multiple_of(c * AW, AW), AW)
        gq_s[:, part] = mm_nt(ut_s[...], dgu_s[part, :])
    loop(3, dwqkv)
    red[WQKV].d_send()
    red[WI].z2()
    red[WO].z2()
    bias_sums(dacc_s, p_s.at[0, 0])
    sm_s[0, 0:1, 0:256] = jnp.sum(p_s[0, 0].T, axis=0, keepdims=True)
    sm_s[0, 0:1, 256:512] = jnp.zeros((1, 256), F32)
    sm_s[0, 1:2, :] = jnp.sum(dga_s[...].T, axis=0, keepdims=True)
    sm_s[0, 2:3, :] = jnp.sum(dgm_s[...].T, axis=0, keepdims=True)
    sm_s[0, 3:8, :] = jnp.zeros((5, 512), F32)
    small.advance(0)
    red[WQKV].xy1()
    small.advance(1)
    red[WQKV].xy2()
    small.advance(2)
    red[WQKV].z1()
    small.advance(3)
    red[WQKV].z2()
    small_ref[...] = small.finish()
    for a in (WF, WI, WO):
        red[a].finish()
    finals = [(out_f, df_ref), (out_i.at[:, pl.ds(0, FF)], di0_ref), (out_i.at[:, pl.ds(FF, FF)], di1_ref), (out_o, do_ref),
              (out_q.at[:, pl.ds(0, AW)], dq_ref), (out_q.at[:, pl.ds(AW, AW)], dk_ref), (out_q.at[:, pl.ds(2 * AW, AW)], dv_ref)]
    finals = [pltpu.make_async_copy(src, dst, out_sem.at[i]) for i, (src, dst) in enumerate(finals)]
    for copy in finals[:4]:
        copy.start()
    red[WQKV].finish()
    for copy in finals[4:]:
        copy.start()
    for copy in finals:
        copy.wait()
    for r in range(ROWS):
        y_copy(r).wait()
    gather.drain()
    for g in red:
        g.drain()
    small.drain()


def local_layer(x_in, positions, segments, rel_bias, gain_attn, gain_mlp, wq, wk, wv, wo, wi0, wi1, wf, grad_out):
    vmem = pl.BlockSpec(memory_space=pltpu.VMEM)
    hbm = pl.BlockSpec(memory_space=pl.ANY)

    def bufs(shape_of, dtype):
        return [pltpu.VMEM(shape_of(r, c), dtype) for r, c in SHARD]

    def quarter(r, c):
        return (3, r, 128) if r == 48 else (3, r // 4, c)
    outs = pl.pallas_call(
        layer_kernel,
        out_shape=[jax.ShapeDtypeStruct((TOK, DM), BF16), jax.ShapeDtypeStruct((8, 512), F32)]
        + [jax.ShapeDtypeStruct(w.shape, BF16) for w in (wq, wk, wv, wo, wi0, wi1, wf)],
        in_specs=[hbm] + [vmem] * 5 + [hbm] * 8,
        out_specs=[hbm, vmem] + [hbm] * 7,
        scratch_shapes=[
            pltpu.VMEM((8, 128), F32), pltpu.VMEM((128, 128), F32), pltpu.VMEM((DM, 128), F32), pltpu.VMEM((DM, 128), F32),
            pltpu.VMEM((DM, 3 * AW), BF16), pltpu.VMEM((AW, DM), BF16), pltpu.VMEM((DM, 2 * FF), BF16), pltpu.VMEM((FF, DM), BF16),
            pltpu.VMEM((3 * AW, DM), BF16), pltpu.VMEM((DM, AW), BF16), pltpu.VMEM((2 * FF, DM), BF16), pltpu.VMEM((DM, FF), BF16),
            pltpu.VMEM((DM, TOK), BF16), pltpu.VMEM((3 * AW, TOK), BF16),
            pltpu.VMEM((HEADS, ROWS, SEQ, SEQ), F32), pltpu.VMEM((AW, TOK), BF16),
            pltpu.VMEM((DM, TOK), BF16), pltpu.VMEM((DM, TOK), BF16), pltpu.VMEM((FF, TOK), BF16), pltpu.VMEM((2 * FF, TOK), BF16),
            pltpu.VMEM((DM, TOK), BF16), pltpu.VMEM((HEADS, SEQ, SEQ), F32), pltpu.VMEM((DM, 128), F32), pltpu.VMEM((DM, 128), F32),
            pltpu.VMEM((TOK, DM), BF16)]
        + bufs(lambda r, c: (8 * r, c), F32) + bufs(lambda r, c: (4, r, c), F32) + bufs(lambda r, c: (4, r // 2, c), F32)
        + bufs(lambda r, c: (2, r // 2, c), F32) + bufs(quarter, F32) + bufs(lambda r, c: (r, c), BF16)
        + [pltpu.VMEM((3, 8, 512), F32), pltpu.VMEM((3, 8, 512), F32), pltpu.VMEM((4, 8, 512), F32),
           pltpu.SemaphoreType.DMA((3, ROWS)), pltpu.SemaphoreType.DMA((7,)), pltpu.SemaphoreType.DMA((7,)), pltpu.SemaphoreType.DMA((49,)), pltpu.SemaphoreType.DMA((49,)),
           pltpu.SemaphoreType.DMA((4 * NSEM + 6,)), pltpu.SemaphoreType.DMA((4 * NSEM + 6,))],
        compiler_params=pltpu.CompilerParams(vmem_limit_bytes=67043328, collective_id=0, has_side_effects=True),
        name='layer',
    )(x_in.reshape(TOK, DM), positions.reshape(ROWS, 1, SEQ), segments.reshape(ROWS, 1, SEQ), rel_bias,
      gain_attn.reshape(1, DM), gain_mlp.reshape(1, DM), wq, wk, wv, wo, wi0, wi1, wf, grad_out.reshape(TOK, DM))
    y, small = outs[0], outs[1]
    db = small[0, 0:256].reshape(32, 8)[:, :HEADS]
    return (y.reshape(ROWS, SEQ, DM), db, small[1], small[2]) + tuple(outs[2:])


def solution(mesh):
    row_spec = P(ROW_AXES)
    whole = P()
    part_spec = P('fsdp')
    in_specs = (row_spec, row_spec, row_spec, whole, whole, whole) + (part_spec,) * 7 + (row_spec,)
    out_specs = (row_spec, whole, whole, whole) + (part_spec,) * 7
    return jax.shard_map(local_layer, mesh=mesh, in_specs=in_specs, out_specs=out_specs, check_vma=False)
```

```python
import functools

import jax
import jax.numpy as jnp
from jax import lax
from jax.experimental import pallas as pl
from jax.experimental.pallas import tpu as pltpu
from jax.sharding import PartitionSpec as P

EPSILON = 1e-6
NEG_BIG = -1e9
THRESHOLDS = (12, 16, 23, 32, 46, 64, 91)
ROW_AXES = ('dp', 'fsdp')
ROWS, SEQ, DM, HEADS, HD, FF = 6, 256, 512, 6, 64, 1024
TOK = ROWS * SEQ
AW = HEADS * HD
F32, BF16 = jnp.float32, jnp.bfloat16


def mm(a, b):
    return lax.dot_general(a, b, (((1,), (0,)), ((), ())), preferred_element_type=F32)


def mm_nt(a, b):
    return lax.dot_general(a, b, (((1,), (1,)), ((), ())), preferred_element_type=F32)


def mm_tn(a, b):
    return lax.dot_general(a, b, (((0,), (0,)), ((), ())), preferred_element_type=F32)


def split3(v):
    hi = v.astype(BF16)
    rest = v - hi.astype(F32)
    mid = rest.astype(BF16)
    lo = (rest - mid.astype(F32)).astype(BF16)
    return hi, mid, lo


def tok_slice(r):
    return pl.ds(pl.multiple_of(r * SEQ, SEQ), SEQ)


def rel_class(diff):
    m = jnp.abs(diff)
    e = jnp.minimum(m, 8.0)
    for bound in THRESHOLDS:
        e = e + jnp.where(m >= bound, 1.0, 0.0)
    return e + jnp.where(diff > 0, 16.0, 0.0)


def setup_small(relb_ref, ga_ref, gm_ref, tab_s, pad_s, ga_s, gm_s):
    pad_s[...] = jnp.zeros_like(pad_s)
    pad_s[0:HEADS, 0:32] = relb_ref[...]
    t = pad_s[0:8, :]
    lane = lax.broadcasted_iota(jnp.int32, t.shape, 1)
    tab_s[...] = jnp.where(lane < 32, t, pltpu.roll(t, 32, 1) + NEG_BIG)
    ga_s[...] = jnp.broadcast_to(ga_ref[...], (128, DM)).T
    gm_s[...] = jnp.broadcast_to(gm_ref[...], (128, DM)).T


def wide(col128):
    return jnp.concatenate([col128, col128], axis=1)


def prep_row(r, x_ref, pos_ref, seg_ref, ga_s, xt_s, at_s, idx_s):
    tok = tok_slice(r)
    xt = x_ref[tok, :].T
    xt_s[:, tok] = xt
    xf = xt.astype(F32)
    inv = lax.rsqrt(jnp.mean(xf * xf, axis=0, keepdims=True) + EPSILON)
    at_s[:, tok] = (xf * inv * wide(ga_s[...])).astype(BF16)
    code = (seg_ref[pl.ds(r, 1), :] * 1024 + pos_ref[pl.ds(r, 1), :]).astype(F32)
    code = jnp.broadcast_to(code, (SEQ, SEQ))
    diff = code.T - code
    idx_s[r] = rel_class(diff) + jnp.where(jnp.abs(diff) >= 512.0, 32.0, 0.0)


def attn_fwd_row(r, tab_s, idx_s, wqkvt_s, at_s, qkv_s, p_s, ctx_s):
    tok = tok_slice(r)
    qkv = mm(wqkvt_s[...], at_s[:, tok]).astype(BF16)
    qkv_s[:, tok] = qkv
    idx = idx_s[r].astype(jnp.int32)

    def scores(h):
        return mm_tn(qkv[AW + h * HD:AW + (h + 1) * HD], qkv[h * HD:(h + 1) * HD])
    s_next = scores(0)
    for h in range(HEADS):
        s = s_next
        if h + 1 < HEADS:
            s_next = scores(h + 1)
        table = jnp.broadcast_to(tab_s[h:h + 1, :], (SEQ, 128))
        s = s + jnp.concatenate([jnp.take_along_axis(table, idx[:, 0:128], axis=1),
                                 jnp.take_along_axis(table, idx[:, 128:256], axis=1)], axis=1)
        p = jnp.exp(s - jnp.max(s, axis=0, keepdims=True))
        p = p * (1.0 / jnp.sum(p, axis=0, keepdims=True))
        p_s[h, r] = p
        ctx_s[h * HD:(h + 1) * HD, tok] = mm(qkv[2 * AW + h * HD:2 * AW + (h + 1) * HD], p.astype(BF16)).astype(BF16)


def mlp_up_row(r, go_ref, gm_s, wot_s, wit_s, wf_s, xt_s, ctx_s, got_s, ut_s, zt_s, dgu_s, h_s):
    tok = tok_slice(r)
    ht = (xt_s[:, tok].astype(F32) + mm(wot_s[...], ctx_s[:, tok])).astype(BF16)
    h_s[:, tok] = ht
    hf = ht.astype(F32)
    inv = lax.rsqrt(jnp.mean(hf * hf, axis=0, keepdims=True) + EPSILON)
    ut = (hf * inv * wide(gm_s[...])).astype(BF16)
    ut_s[:, tok] = ut
    got = go_ref[tok, :].T
    got_s[:, tok] = got
    step = 256

    def products(f):
        return mm(wit_s[f:f + step, :], ut), mm(wit_s[FF + f:FF + f + step, :], ut), mm(wf_s[f:f + step, :], got)
    nxt = products(0)
    for f in range(0, FF, step):
        gate, up, dz = nxt
        if f + step < FF:
            nxt = products(f + step)
        dz = dz.astype(BF16).astype(F32)
        sg = 1.0 / (1.0 + jnp.exp(-gate))
        silu = gate * sg
        zt_s[f:f + step, tok] = (silu * up).astype(BF16)
        dgu_s[f:f + step, tok] = (dz * up * (sg * (1.0 + gate * (1.0 - sg)))).astype(BF16)
        dgu_s[FF + f:FF + f + step, tok] = (dz * silu).astype(BF16)


def mlp_down_row(r, y_ref, gm_s, wft_s, wi_s, got_s, zt_s, dgu_s, h_s, dgm_s):
    tok = tok_slice(r)
    hf = h_s[:, tok].astype(F32)
    inv = lax.rsqrt(jnp.mean(hf * hf, axis=0, keepdims=True) + EPSILON)
    gm = wide(gm_s[...])
    du = mm(wi_s[...], dgu_s[:, tok])
    yt = (hf + mm(wft_s[...], zt_s[:, tok])).astype(BF16)
    y_ref[tok, :] = yt.T
    du = du.astype(BF16).astype(F32)
    hn = hf * inv
    dg = du * hn
    dgm_s[...] += dg[:, 0:128] + dg[:, 128:256]
    dug = du * gm
    dhn = inv * (dug - hn * jnp.mean(dug * hn, axis=0, keepdims=True))
    h_s[:, tok] = (got_s[:, tok].astype(F32) + dhn).astype(BF16)


def attn_bwd_row(r, ga_s, wo_s, xt_s, at_s, qkv_s, p_s, dh_s, dqkv_s):
    tok = tok_slice(r)
    dct = mm(wo_s[...], dh_s[:, tok]).astype(BF16)
    qkv = qkv_s[:, tok]

    def dprob(h):
        return mm_tn(qkv[2 * AW + h * HD:2 * AW + (h + 1) * HD], dct[h * HD:(h + 1) * HD])
    dp_next = dprob(0)
    for h in range(HEADS):
        dp = dp_next
        if h + 1 < HEADS:
            dp_next = dprob(h + 1)
        p = p_s[h, r]
        dqkv_s[2 * AW + h * HD:2 * AW + (h + 1) * HD, tok] = mm_nt(dct[h * HD:(h + 1) * HD], p.astype(BF16)).astype(BF16)
        ds = p * (dp - jnp.sum(dp * p, axis=0, keepdims=True))
        p_s[h, r] = ds
        low = ds.astype(BF16)
        dqkv_s[h * HD:(h + 1) * HD, tok] = mm(qkv[AW + h * HD:AW + (h + 1) * HD], low).astype(BF16)
        dqkv_s[AW + h * HD:AW + (h + 1) * HD, tok] = mm_nt(qkv[h * HD:(h + 1) * HD], low).astype(BF16)
    xf = xt_s[:, tok].astype(F32)
    inv = lax.rsqrt(jnp.mean(xf * xf, axis=0, keepdims=True) + EPSILON)
    at_s[:, tok] = (xf * inv * wide(ga_s[...])).astype(BF16)


def bias_row(r, pos_ref, p_s, dacc_s):
    pos = pos_ref[pl.ds(r, 1), :]
    onehot = jnp.where(lax.broadcasted_iota(jnp.int32, (SEQ, SEQ), 0) == pos, 1.0, 0.0).astype(BF16)

    def first(h):
        hi, mid, lo = split3(p_s[h, r])
        return mm(onehot, hi) + mm(onehot, mid) + mm(onehot, lo)
    nxt = first(0)
    for h in range(HEADS):
        t = nxt
        if h + 1 < HEADS:
            nxt = first(h + 1)
        hi, mid, lo = split3(t)
        dacc_s[h] += mm_nt(hi, onehot) + mm_nt(mid, onehot) + mm_nt(lo, onehot)


def gain_row(r, wqkv_s, xt_s, dqkv_s, dga_s):
    tok = tok_slice(r)
    dn = mm(wqkv_s[...], dqkv_s[0:3 * AW, tok]).astype(BF16).astype(F32)
    xf = xt_s[:, tok].astype(F32)
    inv = lax.rsqrt(jnp.mean(xf * xf, axis=0, keepdims=True) + EPSILON)
    dg = dn * (xf * inv)
    dga_s[...] += dg[:, 0:128] + dg[:, 128:256]


def bias_sums(dacc_s, db_s):
    sub = lax.broadcasted_iota(jnp.int32, (8, SEQ), 0)
    lane = lax.broadcasted_iota(jnp.int32, (8, SEQ), 1)
    below = (sub - lane).astype(F32)
    above = jnp.where(lane <= sub, sub - lane, sub - lane + SEQ).astype(F32)
    cls_a, cls_b = rel_class(above), rel_class(below)

    def head(h):
        acc_a = jnp.zeros((8, SEQ), F32)
        acc_b = jnp.zeros((8, SEQ), F32)
        for t in range(SEQ // 8):
            d = dacc_s[h, 8 * t:8 * t + 8, :]
            keep = lane <= sub + 8 * t
            a, b = jnp.where(keep, d, 0.0), jnp.where(keep, 0.0, d)
            if t > 0:
                a, b = pltpu.roll(a, SEQ - 8 * t, 1), pltpu.roll(b, SEQ - 8 * t, 1)
            acc_a, acc_b = acc_a + a, acc_b + b
        for c in range(32):
            if c < 16:
                v = jnp.where(cls_b == float(c), acc_b, 0.0)
                if c == 0:
                    v = v + jnp.where(cls_a == 0.0, acc_a, 0.0)
            else:
                v = jnp.where(cls_a == float(c), acc_a, 0.0)
            db_s[pl.ds(h * 32 + c, 1), :] = jnp.sum(v, axis=0, keepdims=True)
    loop(HEADS, head)


def loop(n, fn):
    def body(i, carry):
        fn(i)
        return carry
    lax.fori_loop(0, n, body, 0)


MESH = pl.DeviceIdType.MESH
SHARD = ((128, 512), (64, 2048), (48, 512), (64, 1152))
WF, WI, WO, WQKV = 0, 1, 2, 3
NSEM = 16


def remote(src, dst, send, recv, i, dev):
    return pltpu.make_async_remote_copy(src_ref=src, dst_ref=dst, send_sem=send.at[i], recv_sem=recv.at[i],
                                        device_id=dev, device_id_type=MESH)


class Place:
    def __init__(self):
        self.f = lax.axis_index('fsdp')
        self.z = lax.axis_index('dp')
        self.c = lax.rem(self.f, 2)
        self.k = self.f // 2
        self.x = lax.rem(self.k, 2)
        self.y = self.k // 2
        self.kx = self.k + 1 - 2 * self.x
        self.ky = self.k + 2 - 4 * self.y
        self.kd = 3 - self.k
        self.sib = {'fsdp': self.f + 1 - 2 * self.c}
        self.nx = {'fsdp': 2 * self.kx + self.c}
        self.ny = {'fsdp': 2 * self.ky + self.c}
        self.nd = {'fsdp': 2 * self.kd + self.c}
        self.up = [lax.rem(self.z + j, 4) for j in (1, 2, 3)]
        self.nz = [{'dp': u} for u in self.up]


class Gather:
    N = 9

    def __init__(self, at, parts, fulls, own, send, recv):
        self.at, self.parts, self.fulls, self.own, self.send, self.recv = at, parts, fulls, own, send, recv

    def view(self, w, f, h=None):
        full, col = self.fulls[w]
        rows, cols = self.parts[w].shape
        off = f * rows
        if h is not None:
            cut = (rows // 2 + 15) // 16 * 16
            off = off + h * cut
            rows = cut if h == 0 else rows - cut
        return full.at[pl.ds(pl.multiple_of(off, 16), rows), pl.ds(col, cols)]

    def load(self, w):
        return pltpu.make_async_copy(self.parts[w], self.view(w, self.at.f), self.own.at[w])

    def direct(self, w, j):
        at = self.at
        v = self.view(w, at.f)
        return remote(v, v, self.send, self.recv, w * self.N + j, (at.nx, at.ny, at.nd, at.sib)[j])

    def forward(self, w, j):
        at = self.at
        v = self.view(w, 2 * (at.kx, at.ky, at.kd)[j] + at.c)
        return remote(v, v, self.send, self.recv, w * self.N + 4 + j, at.sib)

    def diag(self, w, h):
        at = self.at
        v = self.view(w, 2 * (at.kx, at.ky)[h] + at.c, h)
        return remote(v, v, self.send, self.recv, w * self.N + 7 + h, (at.ny, at.nx)[h])

    def begin(self, ws, js):
        for w in ws:
            self.load(w).wait()
            for j in js:
                self.direct(w, j).start()

    def relay(self, ws):
        for w in ws:
            for j in (0, 1, 2):
                self.direct(w, j).wait_recv()
                self.forward(w, j).start()

    def relay1(self, ws):
        for w in ws:
            for j in (0, 1):
                self.direct(w, j).wait_recv()
                self.diag(w, j).start()
                self.forward(w, j).start()

    def relay2(self, ws):
        for w in ws:
            self.diag(w, 0).wait_recv()
            self.diag(w, 1).wait_recv()
            self.forward(w, 2).start()

    def finish(self, ws):
        for w in ws:
            self.direct(w, 3).wait_recv()
            for j in (0, 1, 2):
                self.forward(w, j).wait_recv()

    def drain(self, ws, halves):
        for w in ws:
            for j in (0, 1, 3) if halves else (0, 1, 2, 3):
                self.direct(w, j).wait_send()
            for j in range(3):
                self.forward(w, j).wait_send()
            if halves:
                self.diag(w, 0).wait_send()
                self.diag(w, 1).wait_send()


class Reduce:
    def __init__(self, a, at, acc, rd, r1, r2, rz, out, send, recv):
        self.a, self.at, self.acc, self.rd, self.r1, self.r2, self.rz, self.out = a, at, acc, rd, r1, r2, rz, out
        self.send, self.recv = send, recv
        self.rows, self.cols = SHARD[a]
        self.half = self.rows // 2

    def part(self, k, c, h=None):
        n = self.rows if h is None else self.half
        off = (2 * k + c) * self.rows + (0 if h is None else h * self.half)
        return self.acc.at[pl.ds(pl.multiple_of(off, 8), n), :]

    def copy(self, src, dst, i, dev):
        return remote(src, dst, self.send, self.recv, self.a * NSEM + i, dev)

    def d_copy(self, i):
        at = self.at
        k = (at.kd, at.kx, at.ky, at.k)[i]
        return self.copy(self.part(k, 1 - at.c), self.rd.at[i], i, at.sib)

    def xy1_copy(self, i):
        at = self.at
        k, h, dev = ((at.kx, 0, at.nx), (at.kd, 0, at.nx), (at.ky, 1, at.ny), (at.kd, 1, at.ny))[i]
        return self.copy(self.part(k, at.c, h), self.r1.at[i], 4 + i, dev)

    def xy2_copy(self, i):
        at = self.at
        k, h, dev = ((at.ky, 0, at.ny), (at.kx, 1, at.nx))[i]
        return self.copy(self.part(k, at.c, h), self.r2.at[i], 8 + i, dev)

    def quarter(self, z, base):
        if self.rows == 48:
            return pl.ds(base, self.rows), pl.ds(pl.multiple_of(z * 128, 128), 128)
        n = self.rows // 4
        return pl.ds(pl.multiple_of(base + z * n, 16), n), slice(None)

    def z1_copy(self, j):
        at = self.at
        rows, cols = self.quarter(at.up[j], pl.multiple_of(at.f * self.rows, 16))
        return self.copy(self.acc.at[rows, cols], self.rz.at[j], 10 + j, at.nz[j])

    def z2_copy(self, j):
        at = self.at
        rows, cols = self.quarter(at.z, 0)
        v = self.out.at[rows, cols]
        return self.copy(v, v, 13 + j, at.nz[j])

    def d_send(self):
        for i in range(4):
            self.d_copy(i).start()

    def add(self, view, buf):
        view[...] = view[...] + buf[...]

    def xy1(self):
        at = self.at
        for i, k in enumerate((at.kd, at.kx, at.ky, at.k)):
            self.d_copy(i).wait_recv()
            self.add(self.part(k, at.c), self.rd.at[i])
        for i in (0, 2, 1, 3):
            self.xy1_copy(i).start()

    def xy2(self):
        at = self.at
        for i, (k, h) in ((1, (at.ky, 0)), (3, (at.kx, 1)), (0, (at.k, 0)), (2, (at.k, 1))):
            self.xy1_copy(i).wait_recv()
            self.add(self.part(k, at.c, h), self.r1.at[i])
            if i == 1:
                self.xy2_copy(0).start()
            if i == 3:
                self.xy2_copy(1).start()

    def z1(self):
        at = self.at
        for i in range(2):
            self.xy2_copy(i).wait_recv()
            self.add(self.part(at.k, at.c, i), self.r2.at[i])
        for j in (1, 0, 2):
            self.z1_copy(j).start()

    def z2(self):
        at = self.at
        rows, cols = self.quarter(at.z, pl.multiple_of(at.f * self.rows, 16))
        total = self.acc[rows, cols]
        for j in range(3):
            self.z1_copy(j).wait_recv()
            total = total + self.rz[j]
        rows, cols = self.quarter(at.z, 0)
        self.out[rows, cols] = total.astype(BF16)
        for j in (1, 0, 2):
            self.z2_copy(j).start()

    def finish(self):
        for j in range(3):
            self.z2_copy(j).wait_recv()

    def drain(self):
        for i in range(4):
            self.d_copy(i).wait_send()
            self.xy1_copy(i).wait_send()
        for i in range(2):
            self.xy2_copy(i).wait_send()
        for i in range(3):
            self.z1_copy(i).wait_send()
            self.z2_copy(i).wait_send()


class Small:
    def __init__(self, at, sm, smr, smz, send, recv):
        self.at, self.sm, self.smr, self.smz, self.send, self.recv = at, sm, smr, smz, send, recv
        self.base = 4 * NSEM

    def step(self, i):
        at = self.at
        return remote(self.sm.at[i], self.smr.at[i], self.send, self.recv, self.base + i, (at.sib, at.nx, at.ny)[i])

    def zcopy(self, j):
        v = self.smz.at[self.at.z]
        return remote(v, v, self.send, self.recv, self.base + 3 + j, self.at.nz[j])

    def advance(self, i):
        if i > 0:
            self.step(i - 1).wait_recv()
            total = self.sm[i - 1] + self.smr[i - 1]
            if i < 3:
                self.sm[i] = total
            else:
                self.smz[self.at.z] = total
        if i < 3:
            self.step(i).start()
        else:
            for j in range(3):
                self.zcopy(j).start()

    def finish(self):
        for j in range(3):
            self.zcopy(j).wait_recv()
        return (self.smz[0] + self.smz[1]) + (self.smz[2] + self.smz[3])

    def drain(self):
        for i in range(3):
            self.step(i).wait_send()
            self.zcopy(i).wait_send()


def layer_kernel(x_hbm, pos_ref, seg_ref, relb_ref, ga_ref, gm_ref, wq_ref, wk_ref, wv_ref, wo_ref, wi0_ref, wi1_ref, wf_ref, go_hbm,
                 y_hbm, small_ref, dq_ref, dk_ref, dv_ref, do_ref, di0_ref, di1_ref, df_ref,
                 tab_s, pad_s, ga_s, gm_s, wqkv_s, wo_s, wi_s, wf_s, wqkvt_s, wot_s, wit_s, wft_s, xt_s, qkv_s, p_s, ctx_s,
                 got_s, ut_s, zt_s, dgu_s, dh_s, dacc_s, dga_s, dgm_s, io_s,
                 gf_s, gi_s, go_s, gq_s, rd_f, rd_i, rd_o, rd_q, r1_f, r1_i, r1_o, r1_q, r2_f, r2_i, r2_o, r2_q,
                 rz_f, rz_i, rz_o, rz_q, out_f, out_i, out_o, out_q, sm_s, smr_s, smz_s,
                 io_sem, out_sem, ag_own, ag_send, ag_recv, rs_send, rs_recv):
    at = Place()
    barrier = pltpu.get_barrier_semaphore()
    peers = [at.sib, at.nx, at.ny, at.nd] + at.nz
    for dev in peers:
        pl.semaphore_signal(barrier, inc=1, device_id=dev, device_id_type=MESH)

    def rows_of(r):
        return pl.ds(pl.multiple_of(r * SEQ, SEQ), SEQ)

    def x_copy(r):
        return pltpu.make_async_copy(x_hbm.at[rows_of(r), :], io_s.at[rows_of(r), :], io_sem.at[0, r])

    def go_copy(r):
        return pltpu.make_async_copy(go_hbm.at[rows_of(r), :], io_s.at[rows_of(r), :], io_sem.at[1, r])

    def y_copy(r):
        return pltpu.make_async_copy(io_s.at[rows_of(r), :], y_hbm.at[rows_of(r), :], io_sem.at[2, r])

    gather = Gather(at, (wq_ref, wk_ref, wv_ref, wo_ref, wi0_ref, wi1_ref, wf_ref),
                    ((wqkv_s, 0), (wqkv_s, AW), (wqkv_s, 2 * AW), (wo_s, 0), (wi_s, 0), (wi_s, FF), (wf_s, 0)), ag_own, ag_send, ag_recv)
    for w in range(7):
        gather.load(w).start()
    for r in range(ROWS):
        x_copy(r).start()
    pl.semaphore_wait(barrier, len(peers))
    first, rest = (0, 1, 2), (3, 4, 5, 6)
    gather.begin(first, (2, 0, 1, 3))
    gather.begin(rest, (0, 1, 3))
    setup_small(relb_ref, ga_ref, gm_ref, tab_s, pad_s, ga_s, gm_s)
    dgm_s[...] = jnp.zeros_like(dgm_s)
    dga_s[...] = jnp.zeros_like(dga_s)

    def prep(r):
        x_copy(r).wait()
        prep_row(r, io_s, pos_ref, seg_ref, ga_s, xt_s, ut_s, dacc_s)
        go_copy(r).start()
    loop(ROWS, prep)
    gather.relay(first)
    gather.finish(first)
    wqkvt_s[...] = wqkv_s[...].T

    def fwd(r):
        attn_fwd_row(r, tab_s, dacc_s, wqkvt_s, ut_s, qkv_s, p_s, ctx_s)

        @pl.when(r == 2)
        def _():
            gather.relay1((3, 4))

        @pl.when(r == 4)
        def _():
            gather.relay1((5, 6))

        @pl.when(r == 5)
        def _():
            gather.relay2((3, 4))
    loop(ROWS, fwd)
    gather.relay2((5, 6))
    gather.finish((3, 4))
    wot_s[...] = wo_s[...].T
    wit_s[0:FF, :] = wi_s[:, 0:FF].T
    gather.finish((5, 6))
    wit_s[FF:2 * FF, :] = wi_s[:, FF:2 * FF].T
    wft_s[...] = wf_s[...].T

    def mlp_up(r):
        go_copy(r).wait()
        mlp_up_row(r, io_s, gm_s, wot_s, wit_s, wf_s, xt_s, ctx_s, got_s, ut_s, zt_s, dgu_s, dh_s)
    loop(ROWS, mlp_up)

    red = [Reduce(WF, at, gf_s, rd_f, r1_f, r2_f, rz_f, out_f, rs_send, rs_recv),
           Reduce(WI, at, gi_s, rd_i, r1_i, r2_i, rz_i, out_i, rs_send, rs_recv),
           Reduce(WO, at, go_s, rd_o, r1_o, r2_o, rz_o, out_o, rs_send, rs_recv),
           Reduce(WQKV, at, gq_s, rd_q, r1_q, r2_q, rz_q, out_q, rs_send, rs_recv)]
    small = Small(at, sm_s, smr_s, smz_s, rs_send, rs_recv)

    def cols(c, n=256):
        return pl.ds(pl.multiple_of(c * n, n), n)

    def dwf(c):
        gf_s[:, cols(c)] = mm_nt(zt_s[...], got_s[cols(c), :])
    loop(2, dwf)
    red[WF].d_send()

    def dwi(c):
        gi_s[:, cols(c)] = mm_nt(ut_s[...], dgu_s[cols(c), :])
    loop(8, dwi)
    red[WI].d_send()
    red[WF].xy1()

    def mlp_down(r):
        mlp_down_row(r, io_s, gm_s, wft_s, wi_s, got_s, zt_s, dgu_s, dh_s, dgm_s)
        y_copy(r).start()

        @pl.when(r == 2)
        def _():
            red[WI].xy1()
    loop(ROWS, mlp_down)
    red[WF].xy2()

    def dwo(c):
        go_s[:, cols(c)] = mm_nt(ctx_s[...], dh_s[cols(c), :])
    loop(2, dwo)
    red[WO].d_send()
    dacc_s[...] = jnp.zeros_like(dacc_s)

    def bwd(r):
        attn_bwd_row(r, ga_s, wo_s, xt_s, ut_s, qkv_s, p_s, dh_s, dgu_s)

        @pl.when(r == 1)
        def _():
            red[WO].xy1()
    loop(ROWS, bwd)

    def dwqkv(c):
        gq_s[:, cols(c, AW)] = mm_nt(ut_s[...], dgu_s[cols(c, AW), :])
    loop(3, dwqkv)
    red[WQKV].d_send()
    red[WI].xy2()

    def tail(r):
        bias_row(r, pos_ref, p_s, dacc_s)
        gain_row(r, wqkv_s, xt_s, dgu_s, dga_s)

        @pl.when(r == 0)
        def _():
            red[WQKV].xy1()
            red[WF].z1()

        @pl.when(r == 1)
        def _():
            red[WO].xy2()

        @pl.when(r == 3)
        def _():
            red[WI].z1()
            red[WF].z2()

        @pl.when(r == 4)
        def _():
            red[WQKV].xy2()
            red[WO].z1()
    loop(ROWS, tail)
    db_s = p_s.at[0, 0]
    db_s[...] = jnp.zeros_like(db_s)
    bias_sums(dacc_s, db_s)
    sm_s[0, 0:1, 0:256] = jnp.sum(p_s[0, 0].T, axis=0, keepdims=True)
    sm_s[0, 0:1, 256:512] = jnp.zeros((1, 256), F32)
    sm_s[0, 1:2, :] = jnp.sum(dga_s[...].T, axis=0, keepdims=True)
    sm_s[0, 2:3, :] = jnp.sum(dgm_s[...].T, axis=0, keepdims=True)
    sm_s[0, 3:8, :] = jnp.zeros((5, 512), F32)
    small.advance(0)
    red[WQKV].z1()
    small.advance(1)
    red[WI].z2()
    small.advance(2)
    red[WO].z2()
    small.advance(3)
    red[WQKV].z2()
    small_ref[...] = small.finish()
    for a in (WF, WI, WO):
        red[a].finish()
    finals = [(out_f, df_ref), (out_i.at[:, pl.ds(0, FF)], di0_ref), (out_i.at[:, pl.ds(FF, FF)], di1_ref), (out_o, do_ref),
              (out_q.at[:, pl.ds(0, AW)], dq_ref), (out_q.at[:, pl.ds(AW, AW)], dk_ref), (out_q.at[:, pl.ds(2 * AW, AW)], dv_ref)]
    finals = [pltpu.make_async_copy(src, dst, out_sem.at[i]) for i, (src, dst) in enumerate(finals)]
    for copy in finals[:4]:
        copy.start()
    red[WQKV].finish()
    for copy in finals[4:]:
        copy.start()
    for copy in finals:
        copy.wait()
    for r in range(ROWS):
        y_copy(r).wait()
    gather.drain(first, False)
    gather.drain(rest, True)
    for g in red:
        g.drain()
    small.drain()


def emit_kernel(y_in, small_ref, g0, g1, g2, g3, g4, g5, g6, y_out, db_ref, dga_ref, dgm_ref, o0, o1, o2, o3, o4, o5, o6,
                y_s, b0, b1, b2, b3, b4, b5, b6, in_sem, out_sem):
    pairs = [(y_in.at[pl.ds(r * SEQ, SEQ), :], y_s.at[pl.ds(r * SEQ, SEQ), :], y_out.at[pl.ds(r * SEQ, SEQ), :]) for r in range(ROWS)]
    pairs += list(zip((g0, g1, g2, g3, g4, g5, g6), (b0, b1, b2, b3, b4, b5, b6), (o0, o1, o2, o3, o4, o5, o6)))
    ins = [pltpu.make_async_copy(a, b, in_sem.at[i]) for i, (a, b, _) in enumerate(pairs)]
    outs = [pltpu.make_async_copy(b, c, out_sem.at[i]) for i, (_, b, c) in enumerate(pairs)]
    for copy in ins:
        copy.start()
    for h in range(HEADS):
        db_ref[h:h + 1, :] = small_ref[0:1, h * 32:(h + 1) * 32]
    dga_ref[...] = small_ref[1:2, :]
    dgm_ref[...] = small_ref[2:3, :]
    for i in range(len(pairs)):
        ins[i].wait()
        outs[i].start()
    for copy in outs:
        copy.wait()


def local_layer(x_in, positions, segments, rel_bias, gain_attn, gain_mlp, wq, wk, wv, wo, wi0, wi1, wf, grad_out):
    vmem = pl.BlockSpec(memory_space=pltpu.VMEM)
    hbm = pl.BlockSpec(memory_space=pl.ANY)

    def bufs(shape_of, dtype):
        return [pltpu.VMEM(shape_of(r, c), dtype) for r, c in SHARD]

    def quarter(r, c):
        return (3, r, 128) if r == 48 else (3, r // 4, c)
    outs = pl.pallas_call(
        layer_kernel,
        out_shape=[jax.ShapeDtypeStruct((TOK, DM), BF16), jax.ShapeDtypeStruct((8, 512), F32)]
        + [jax.ShapeDtypeStruct(w.shape, BF16) for w in (wq, wk, wv, wo, wi0, wi1, wf)],
        in_specs=[hbm] + [vmem] * 5 + [hbm] * 8,
        out_specs=[hbm, vmem] + [hbm] * 7,
        scratch_shapes=[
            pltpu.VMEM((8, 128), F32), pltpu.VMEM((128, 128), F32), pltpu.VMEM((DM, 128), F32), pltpu.VMEM((DM, 128), F32),
            pltpu.VMEM((DM, 3 * AW), BF16), pltpu.VMEM((AW, DM), BF16), pltpu.VMEM((DM, 2 * FF), BF16), pltpu.VMEM((FF, DM), BF16),
            pltpu.VMEM((3 * AW, DM), BF16), pltpu.VMEM((DM, AW), BF16), pltpu.VMEM((2 * FF, DM), BF16), pltpu.VMEM((DM, FF), BF16),
            pltpu.VMEM((DM, TOK), BF16), pltpu.VMEM((3 * AW, TOK), BF16),
            pltpu.VMEM((HEADS, ROWS, SEQ, SEQ), F32), pltpu.VMEM((AW, TOK), BF16),
            pltpu.VMEM((DM, TOK), BF16), pltpu.VMEM((DM, TOK), BF16), pltpu.VMEM((FF, TOK), BF16), pltpu.VMEM((2 * FF, TOK), BF16),
            pltpu.VMEM((DM, TOK), BF16), pltpu.VMEM((HEADS, SEQ, SEQ), F32), pltpu.VMEM((DM, 128), F32), pltpu.VMEM((DM, 128), F32),
            pltpu.VMEM((TOK, DM), BF16)]
        + bufs(lambda r, c: (8 * r, c), F32) + bufs(lambda r, c: (4, r, c), F32) + bufs(lambda r, c: (4, r // 2, c), F32)
        + bufs(lambda r, c: (2, r // 2, c), F32) + bufs(quarter, F32) + bufs(lambda r, c: (r, c), BF16)
        + [pltpu.VMEM((3, 8, 512), F32), pltpu.VMEM((3, 8, 512), F32), pltpu.VMEM((4, 8, 512), F32),
           pltpu.SemaphoreType.DMA((3, ROWS)), pltpu.SemaphoreType.DMA((7,)), pltpu.SemaphoreType.DMA((7,)), pltpu.SemaphoreType.DMA((63,)), pltpu.SemaphoreType.DMA((63,)),
           pltpu.SemaphoreType.DMA((4 * NSEM + 6,)), pltpu.SemaphoreType.DMA((4 * NSEM + 6,))],
        compiler_params=pltpu.CompilerParams(vmem_limit_bytes=67043328, collective_id=0, has_side_effects=True),
        name='layer',
    )(x_in.reshape(TOK, DM), positions, segments, rel_bias.T,
      gain_attn.reshape(1, DM), gain_mlp.reshape(1, DM), wq, wk, wv, wo, wi0, wi1, wf, grad_out.reshape(TOK, DM))
    weights = (wq, wk, wv, wo, wi0, wi1, wf)
    outs = pl.pallas_call(
        emit_kernel,
        out_shape=[jax.ShapeDtypeStruct((TOK, DM), BF16), jax.ShapeDtypeStruct((HEADS, 32), F32),
                   jax.ShapeDtypeStruct((1, DM), F32), jax.ShapeDtypeStruct((1, DM), F32)]
        + [jax.ShapeDtypeStruct(w.shape, BF16) for w in weights],
        in_specs=[hbm, vmem] + [hbm] * 7,
        out_specs=[hbm, vmem, vmem, vmem] + [hbm] * 7,
        scratch_shapes=[pltpu.VMEM((TOK, DM), BF16)] + [pltpu.VMEM(w.shape, BF16) for w in weights]
        + [pltpu.SemaphoreType.DMA((ROWS + 7,)), pltpu.SemaphoreType.DMA((ROWS + 7,))],
        name='emit',
    )(*outs)
    y, db, dga, dgm = outs[:4]
    return (y.reshape(ROWS, SEQ, DM), db.T, dga.reshape(DM), dgm.reshape(DM)) + tuple(outs[4:])


def solution(mesh):
    row_spec = P(ROW_AXES)
    whole = P()
    part_spec = P('fsdp')
    in_specs = (row_spec, row_spec, row_spec, whole, whole, whole) + (part_spec,) * 7 + (row_spec,)
    out_specs = (row_spec, whole, whole, whole) + (part_spec,) * 7
    return jax.shard_map(local_layer, mesh=mesh, in_specs=in_specs, out_specs=out_specs, check_vma=False)
```

```python
import functools

import jax
import jax.numpy as jnp
from jax import lax
from jax.experimental import pallas as pl
from jax.experimental.pallas import tpu as pltpu
from jax.sharding import PartitionSpec as P

EPSILON = 1e-6
NEG_BIG = -1e9
THRESHOLDS = (12, 16, 23, 32, 46, 64, 91)
ROW_AXES = ('dp', 'fsdp')
ROWS, SEQ, DM, HEADS, HD, FF = 6, 256, 512, 6, 64, 1024
TOK = ROWS * SEQ
AW = HEADS * HD
F32, BF16 = jnp.float32, jnp.bfloat16


def mm(a, b):
    return lax.dot_general(a, b, (((1,), (0,)), ((), ())), preferred_element_type=F32)


def mm_nt(a, b):
    return lax.dot_general(a, b, (((1,), (1,)), ((), ())), preferred_element_type=F32)


def mm_tn(a, b):
    return lax.dot_general(a, b, (((0,), (0,)), ((), ())), preferred_element_type=F32)


def split3(v):
    hi = v.astype(BF16)
    rest = v - hi.astype(F32)
    mid = rest.astype(BF16)
    lo = (rest - mid.astype(F32)).astype(BF16)
    return hi, mid, lo


def tok_slice(r):
    return pl.ds(pl.multiple_of(r * SEQ, SEQ), SEQ)


def rel_class(diff):
    m = jnp.abs(diff)
    e = jnp.minimum(m, 8.0)
    for bound in THRESHOLDS:
        e = e + jnp.where(m >= bound, 1.0, 0.0)
    return e + jnp.where(diff > 0, 16.0, 0.0)


def setup_small(relb_ref, ga_ref, gm_ref, tab_s, pad_s, ga_s, gm_s):
    pad_s[...] = jnp.zeros_like(pad_s)
    pad_s[0:HEADS, 0:32] = relb_ref[...]
    t = pad_s[0:8, :]
    lane = lax.broadcasted_iota(jnp.int32, t.shape, 1)
    tab_s[...] = jnp.where(lane < 32, t, pltpu.roll(t, 32, 1) + NEG_BIG)
    ga_s[...] = jnp.broadcast_to(ga_ref[...], (128, DM)).T
    gm_s[...] = jnp.broadcast_to(gm_ref[...], (128, DM)).T


def wide(col128):
    return jnp.concatenate([col128, col128], axis=1)


def prep_row(r, x_ref, pos_ref, seg_ref, ga_s, xt_s, at_s, idx_s):
    tok = tok_slice(r)
    xt = x_ref[tok, :].T
    xt_s[:, tok] = xt
    xf = xt.astype(F32)
    inv = lax.rsqrt(jnp.mean(xf * xf, axis=0, keepdims=True) + EPSILON)
    at_s[:, tok] = (xf * inv * wide(ga_s[...])).astype(BF16)
    code = (seg_ref[pl.ds(r, 1), :] * 1024 + pos_ref[pl.ds(r, 1), :]).astype(F32)
    code = jnp.broadcast_to(code, (SEQ, SEQ))
    diff = code.T - code
    idx_s[r] = (rel_class(diff) + jnp.where(jnp.abs(diff) >= 512.0, 32.0, 0.0)).astype(jnp.int32)


def lane_lookup(table, idx):
    dims = lax.GatherDimensionNumbers(offset_dims=(), collapsed_slice_dims=(1,), start_index_map=(1,),
                                      operand_batching_dims=(0,), start_indices_batching_dims=(0,))
    return lax.gather(table, idx[:, :, None], dims, (1, 1), mode='promise_in_bounds')


def qkv_block(r, wqkvt_s, at_s, qkv_s):
    tok = pl.ds(pl.multiple_of(r * 512, 512), 512)
    qkv_s[:, tok] = mm(wqkvt_s[...], at_s[:, tok]).astype(BF16)


def attn_fwd_row(r, tab_s, idx_s, qkv_s, p_s, ctx_s):
    tok = tok_slice(r)
    half = SEQ // 2

    def scores(h):
        kt, qt = qkv_s[AW + h * HD:AW + (h + 1) * HD, tok], qkv_s[h * HD:(h + 1) * HD, tok]
        return [mm_tn(kt, qt[:, 0:half]), mm_tn(kt, qt[:, half:SEQ])]
    s_next = scores(0)
    for h in range(HEADS):
        s_now = s_next
        if h + 1 < HEADS:
            s_next = scores(h + 1)
        table = jnp.broadcast_to(tab_s[h:h + 1, :], (SEQ, 128))
        low = []
        for i in range(2):
            cols = slice(i * half, (i + 1) * half)
            s = s_now[i] + lane_lookup(table, idx_s[r, :, cols])
            p = jnp.exp(s - jnp.max(s, axis=0, keepdims=True))
            p = p * (1.0 / jnp.sum(p, axis=0, keepdims=True))
            p_s[h, r, :, cols] = p
            low.append(p.astype(BF16))
        vt = qkv_s[2 * AW + h * HD:2 * AW + (h + 1) * HD, tok]
        ctx_s[h * HD:(h + 1) * HD, tok] = mm(vt, jnp.concatenate(low, axis=1)).astype(BF16)


def mlp_in_row(r, gm_s, wot_s, xt_s, ctx_s, ut_s, h_s):
    tok = tok_slice(r)
    ht = (xt_s[:, tok].astype(F32) + mm(wot_s[...], ctx_s[:, tok])).astype(BF16)
    h_s[:, tok] = ht
    hf = ht.astype(F32)
    inv = lax.rsqrt(jnp.mean(hf * hf, axis=0, keepdims=True) + EPSILON)
    ut_s[:, tok] = (hf * inv * wide(gm_s[...])).astype(BF16)


def mlp_up_row(r, gm_s, wot_s, wit_s, wf_s, xt_s, ctx_s, got_s, ut_s, zt_s, dgu_s, h_s):
    tok = tok_slice(r)
    ut, got = ut_s[:, tok], got_s[:, tok]
    step = 256

    def products(f):
        return mm(wit_s[f:f + step, :], ut), mm(wit_s[FF + f:FF + f + step, :], ut), mm(wf_s[f:f + step, :], got)
    nxt = products(0)
    mlp_in_row(jnp.minimum(r + 1, ROWS - 1), gm_s, wot_s, xt_s, ctx_s, ut_s, h_s)
    for f in range(0, FF, step):
        gate, up, dz = nxt
        if f + step < FF:
            nxt = products(f + step)
        dz = dz.astype(BF16).astype(F32)
        sg = 1.0 / (1.0 + jnp.exp(-gate))
        silu = gate * sg
        zt_s[f:f + step, tok] = (silu * up).astype(BF16)
        dgu_s[f:f + step, tok] = (dz * up * (sg * (1.0 + gate * (1.0 - sg)))).astype(BF16)
        dgu_s[FF + f:FF + f + step, tok] = (dz * silu).astype(BF16)


def mlp_down_row(r, y_ref, gm_s, wft_s, wi_s, got_s, zt_s, dgu_s, h_s, dgm_s):
    tok = tok_slice(r)
    hf = h_s[:, tok].astype(F32)
    inv = lax.rsqrt(jnp.mean(hf * hf, axis=0, keepdims=True) + EPSILON)
    gm = wide(gm_s[...])
    du = mm(wi_s[...], dgu_s[:, tok])
    yt = (hf + mm(wft_s[...], zt_s[:, tok])).astype(BF16)
    y_ref[tok, :] = yt.T
    du = du.astype(BF16).astype(F32)
    hn = hf * inv
    dg = du * hn
    dgm_s[...] += dg[:, 0:128] + dg[:, 128:256]
    dug = du * gm
    dhn = inv * (dug - hn * jnp.mean(dug * hn, axis=0, keepdims=True))
    h_s[:, tok] = (got_s[:, tok].astype(F32) + dhn).astype(BF16)


def attn_bwd_row(r, ga_s, wo_s, xt_s, at_s, qkv_s, p_s, dh_s, dqkv_s):
    tok = tok_slice(r)
    dct = mm(wo_s[...], dh_s[:, tok]).astype(BF16)
    qkv = qkv_s[:, tok]

    def dprob(h):
        return mm_tn(qkv[2 * AW + h * HD:2 * AW + (h + 1) * HD], dct[h * HD:(h + 1) * HD])
    dp_next = dprob(0)
    for h in range(HEADS):
        dp = dp_next
        if h + 1 < HEADS:
            dp_next = dprob(h + 1)
        p = p_s[h, r]
        dqkv_s[2 * AW + h * HD:2 * AW + (h + 1) * HD, tok] = mm_nt(dct[h * HD:(h + 1) * HD], p.astype(BF16)).astype(BF16)
        ds = p * (dp - jnp.sum(dp * p, axis=0, keepdims=True))
        p_s[h, r] = ds
        low = ds.astype(BF16)
        dqkv_s[h * HD:(h + 1) * HD, tok] = mm(qkv[AW + h * HD:AW + (h + 1) * HD], low).astype(BF16)
        dqkv_s[AW + h * HD:AW + (h + 1) * HD, tok] = mm_nt(qkv[h * HD:(h + 1) * HD], low).astype(BF16)
    xf = xt_s[:, tok].astype(F32)
    inv = lax.rsqrt(jnp.mean(xf * xf, axis=0, keepdims=True) + EPSILON)
    at_s[:, tok] = (xf * inv * wide(ga_s[...])).astype(BF16)


def bias_view(dacc, h):
    return dacc[h // 4].at[(h % 4) * SEQ:(h % 4 + 1) * SEQ, :]


def bias_row(r, pos_ref, p_s, dacc):
    pos = pos_ref[pl.ds(r, 1), :]
    onehot = jnp.where(lax.broadcasted_iota(jnp.int32, (SEQ, SEQ), 0) == pos, 1.0, 0.0).astype(BF16)

    def first(h):
        hi, mid, lo = split3(p_s[h, r])
        return mm(onehot, hi) + mm(onehot, mid) + mm(onehot, lo)
    nxt = first(0)
    for h in range(HEADS):
        t = nxt
        if h + 1 < HEADS:
            nxt = first(h + 1)
        hi, mid, lo = split3(t)
        bias_view(dacc, h)[...] += mm_nt(hi, onehot) + mm_nt(mid, onehot) + mm_nt(lo, onehot)


def gain_row(r, wqkv_s, xt_s, dqkv_s, dga_s):
    tok = tok_slice(r)
    dn = mm(wqkv_s[...], dqkv_s[0:3 * AW, tok]).astype(BF16).astype(F32)
    xf = xt_s[:, tok].astype(F32)
    inv = lax.rsqrt(jnp.mean(xf * xf, axis=0, keepdims=True) + EPSILON)
    dg = dn * (xf * inv)
    dga_s[...] += dg[:, 0:128] + dg[:, 128:256]


def bias_sums(dacc, db_s):
    sub = lax.broadcasted_iota(jnp.int32, (8, SEQ), 0)
    lane = lax.broadcasted_iota(jnp.int32, (8, SEQ), 1)
    below = (sub - lane).astype(F32)
    above = jnp.where(lane <= sub, sub - lane, sub - lane + SEQ).astype(F32)
    cls_a, cls_b = rel_class(above), rel_class(below)

    def head(h, src, first):
        acc_a = jnp.zeros((8, SEQ), F32)
        acc_b = jnp.zeros((8, SEQ), F32)
        for t in range(SEQ // 8):
            d = src[pl.ds(pl.multiple_of(h * SEQ + 8 * t, 8), 8), :]
            keep = lane <= sub + 8 * t
            a, b = jnp.where(keep, d, 0.0), jnp.where(keep, 0.0, d)
            if t > 0:
                a, b = pltpu.roll(a, SEQ - 8 * t, 1), pltpu.roll(b, SEQ - 8 * t, 1)
            acc_a, acc_b = acc_a + a, acc_b + b
        for c in range(32):
            if c < 16:
                v = jnp.where(cls_b == float(c), acc_b, 0.0)
                if c == 0:
                    v = v + jnp.where(cls_a == 0.0, acc_a, 0.0)
            else:
                v = jnp.where(cls_a == float(c), acc_a, 0.0)
            db_s[pl.ds((h + first) * 32 + c, 1), :] = jnp.sum(v, axis=0, keepdims=True)
    loop(4, lambda h: head(h, dacc[0], 0))
    loop(HEADS - 4, lambda h: head(h, dacc[1], 4))


def loop(n, fn):
    def body(i, carry):
        fn(i)
        return carry
    lax.fori_loop(0, n, body, 0)


MESH = pl.DeviceIdType.MESH
SHARD = ((128, 256),) * 2 + ((64, 512),) * 4 + ((48, 512),) + ((64, 384),) * 3
NG = len(SHARD)
PLAN = {
    ('wf', 0): (('d', 0),),
    ('wf', 1): (('d', 1), ('a', 0)),
    ('wi', 0): (('a', 1),),
    ('wi', 1): (('d', 2),),
    ('wi', 3): (('d', 3),),
    ('wi', 5): (('d', 4), ('b', 0)),
    ('wi', 6): (('a', 2),),
    ('wi', 7): (('d', 5),),
    ('down', 0): (('b', 1),),
    ('down', 1): (('y', 0),),
    ('down', 2): (('a', 3),),
    ('down', 3): (('b', 2),),
    ('down', 4): (('y', 1),),
    ('down', 5): (('a', 4), ('z', 0)),
    ('wo', 0): (('d', 6), ('b', 3)),
    ('bwd', 0): (('y', 2),),
    ('bwd', 1): (('a', 5), ('z', 1)),
    ('bwd', 2): (('b', 4),),
    ('bwd', 3): (('y', 3),),
    ('bwd', 4): (('a', 6), ('z', 2)),
    ('bwd', 5): (('b', 5),),
    ('wqkv', 0): (('d', 7), ('y', 4)),
    ('wqkv', 1): (('d', 8), ('a', 7), ('z', 3)),
    ('wqkv', 2): (('d', 9), ('b', 6)),
    ('tail', 0): (('y', 5), ('a', 8)),
    ('tail', 1): (('b', 7), ('y', 6), ('a', 9), ('z', 4)),
    ('tail', 2): (('b', 8),),
    ('tail', 3): (('y', 7), ('z', 5)),
    ('tail', 4): (('b', 9), ('y', 8)),
    ('tail', 5): (('y', 9), ('z', 6), ('z', 7)),
    ('end', 0): (('z', 8), ('z', 9)),
}
NSEM = 16


def remote(src, dst, send, recv, i, dev):
    return pltpu.make_async_remote_copy(src_ref=src, dst_ref=dst, send_sem=send.at[i], recv_sem=recv.at[i],
                                        device_id=dev, device_id_type=MESH)


class Place:
    def __init__(self):
        self.f = lax.axis_index('fsdp')
        self.z = lax.axis_index('dp')
        self.c = lax.rem(self.f, 2)
        self.k = self.f // 2
        self.x = lax.rem(self.k, 2)
        self.y = self.k // 2
        self.kx = self.k + 1 - 2 * self.x
        self.ky = self.k + 2 - 4 * self.y
        self.kd = 3 - self.k
        self.sib = {'fsdp': self.f + 1 - 2 * self.c}
        self.nx = {'fsdp': 2 * self.kx + self.c}
        self.ny = {'fsdp': 2 * self.ky + self.c}
        self.nd = {'fsdp': 2 * self.kd + self.c}
        self.up = [lax.rem(self.z + j, 4) for j in (1, 2, 3)]
        self.nz = [{'dp': u} for u in self.up]


class Gather:
    N = 9

    def __init__(self, at, parts, fulls, own, send, recv):
        self.at, self.parts, self.fulls, self.own, self.send, self.recv = at, parts, fulls, own, send, recv

    def view(self, w, f, h=None):
        full, col = self.fulls[w]
        rows, cols = self.parts[w].shape
        off = f * rows
        if h is not None:
            cut = (rows // 2 + 15) // 16 * 16
            off = off + h * cut
            rows = cut if h == 0 else rows - cut
        return full.at[pl.ds(pl.multiple_of(off, 16), rows), pl.ds(col, cols)]

    def load(self, w):
        return pltpu.make_async_copy(self.parts[w], self.view(w, self.at.f), self.own.at[w])

    def direct(self, w, j):
        at = self.at
        v = self.view(w, at.f)
        return remote(v, v, self.send, self.recv, w * self.N + j, (at.nx, at.ny, at.nd, at.sib)[j])

    def forward(self, w, j):
        at = self.at
        v = self.view(w, 2 * (at.kx, at.ky, at.kd)[j] + at.c)
        return remote(v, v, self.send, self.recv, w * self.N + 4 + j, at.sib)

    def diag(self, w, h):
        at = self.at
        v = self.view(w, 2 * (at.kx, at.ky)[h] + at.c, h)
        return remote(v, v, self.send, self.recv, w * self.N + 7 + h, (at.ny, at.nx)[h])

    def begin(self, ws, js):
        for w in ws:
            self.load(w).wait()
            for j in js:
                self.direct(w, j).start()

    def relay(self, ws):
        for w in ws:
            for j in (0, 1, 2):
                self.direct(w, j).wait_recv()
                self.forward(w, j).start()

    def relay1(self, ws):
        for w in ws:
            for j in (0, 1):
                self.direct(w, j).wait_recv()
                self.diag(w, j).start()
                self.forward(w, j).start()

    def relay2(self, ws):
        for w in ws:
            self.diag(w, 0).wait_recv()
            self.diag(w, 1).wait_recv()
            self.forward(w, 2).start()

    def finish(self, ws):
        for w in ws:
            self.direct(w, 3).wait_recv()
            for j in (0, 1, 2):
                self.forward(w, j).wait_recv()

    def drain(self, ws, halves):
        for w in ws:
            for j in (0, 1, 3) if halves else (0, 1, 2, 3):
                self.direct(w, j).wait_send()
            for j in range(3):
                self.forward(w, j).wait_send()
            if halves:
                self.diag(w, 0).wait_send()
                self.diag(w, 1).wait_send()


class Reduce:
    def __init__(self, a, at, acc, rd, r1, r2, rz, out, send, recv):
        self.a, self.at, self.acc, self.rd, self.r1, self.r2, self.rz, self.out = a, at, acc, rd, r1, r2, rz, out
        self.send, self.recv = send, recv
        self.rows, self.cols = SHARD[a]
        self.half = self.rows // 2

    def part(self, k, c, h=None):
        n = self.rows if h is None else self.half
        off = (2 * k + c) * self.rows + (0 if h is None else h * self.half)
        return self.acc.at[pl.ds(pl.multiple_of(off, 8), n), :]

    def copy(self, src, dst, i, dev):
        return remote(src, dst, self.send, self.recv, self.a * NSEM + i, dev)

    def d_copy(self, i):
        at = self.at
        k = (at.kd, at.kx, at.ky, at.k)[i]
        return self.copy(self.part(k, 1 - at.c), self.rd.at[i], i, at.sib)

    def xy1_copy(self, i):
        at = self.at
        k, h, dev = ((at.kx, 0, at.nx), (at.kd, 0, at.nx), (at.ky, 1, at.ny), (at.kd, 1, at.ny))[i]
        return self.copy(self.part(k, at.c, h), self.r1.at[i], 4 + i, dev)

    def xy2_copy(self, i):
        at = self.at
        k, h, dev = ((at.ky, 0, at.ny), (at.kx, 1, at.nx))[i]
        return self.copy(self.part(k, at.c, h), self.r2.at[i], 8 + i, dev)

    def quarter(self, z, base):
        if self.rows == 48:
            return pl.ds(base, self.rows), pl.ds(pl.multiple_of(z * 128, 128), 128)
        n = self.rows // 4
        return pl.ds(pl.multiple_of(base + z * n, 16), n), slice(None)

    def z1_copy(self, j):
        at = self.at
        rows, cols = self.quarter(at.up[j], pl.multiple_of(at.f * self.rows, 16))
        return self.copy(self.acc.at[rows, cols], self.rz.at[j], 10 + j, at.nz[j])

    def z2_copy(self, j):
        at = self.at
        rows, cols = self.quarter(at.z, 0)
        v = self.out.at[rows, cols]
        return self.copy(v, v, 13 + j, at.nz[j])

    def d_send(self):
        for i in range(4):
            self.d_copy(i).start()

    def add(self, view, buf):
        view[...] = view[...] + buf[...]

    def xy1(self):
        at = self.at
        for i, k in enumerate((at.kd, at.kx, at.ky, at.k)):
            self.d_copy(i).wait_recv()
            self.add(self.part(k, at.c), self.rd.at[i])
        for i in (0, 2, 1, 3):
            self.xy1_copy(i).start()

    def xy2(self):
        at = self.at
        for i, (k, h) in ((1, (at.ky, 0)), (3, (at.kx, 1)), (0, (at.k, 0)), (2, (at.k, 1))):
            self.xy1_copy(i).wait_recv()
            self.add(self.part(k, at.c, h), self.r1.at[i])
            if i == 1:
                self.xy2_copy(0).start()
            if i == 3:
                self.xy2_copy(1).start()

    def z1(self):
        at = self.at
        for i in range(2):
            self.xy2_copy(i).wait_recv()
            self.add(self.part(at.k, at.c, i), self.r2.at[i])
        for j in (1, 0, 2):
            self.z1_copy(j).start()

    def z2(self):
        at = self.at
        rows, cols = self.quarter(at.z, pl.multiple_of(at.f * self.rows, 16))
        total = self.acc[rows, cols]
        for j in range(3):
            self.z1_copy(j).wait_recv()
            total = total + self.rz[j]
        rows, cols = self.quarter(at.z, 0)
        self.out[rows, cols] = total.astype(BF16)
        for j in (1, 0, 2):
            self.z2_copy(j).start()

    def finish(self):
        for j in range(3):
            self.z2_copy(j).wait_recv()

    def drain(self):
        for i in range(4):
            self.d_copy(i).wait_send()
            self.xy1_copy(i).wait_send()
        for i in range(2):
            self.xy2_copy(i).wait_send()
        for i in range(3):
            self.z1_copy(i).wait_send()
            self.z2_copy(i).wait_send()


class Small:
    def __init__(self, at, sm, smr, smz, send, recv):
        self.at, self.sm, self.smr, self.smz, self.send, self.recv = at, sm, smr, smz, send, recv
        self.base = NG * NSEM

    def step(self, i):
        at = self.at
        return remote(self.sm.at[i], self.smr.at[i], self.send, self.recv, self.base + i, (at.sib, at.nx, at.ny)[i])

    def zcopy(self, j):
        v = self.smz.at[self.at.z]
        return remote(v, v, self.send, self.recv, self.base + 3 + j, self.at.nz[j])

    def advance(self, i):
        if i > 0:
            self.step(i - 1).wait_recv()
            total = self.sm[i - 1] + self.smr[i - 1]
            if i < 3:
                self.sm[i] = total
            else:
                self.smz[self.at.z] = total
        if i < 3:
            self.step(i).start()
        else:
            for j in range(3):
                self.zcopy(j).start()

    def finish(self):
        for j in range(3):
            self.zcopy(j).wait_recv()
        return (self.smz[0] + self.smz[1]) + (self.smz[2] + self.smz[3])

    def drain(self):
        for i in range(3):
            self.step(i).wait_send()
            self.zcopy(i).wait_send()


def layer_kernel(x_hbm, pos_ref, seg_ref, relb_ref, ga_ref, gm_ref, wq_ref, wk_ref, wv_ref, wo_ref, wi0_ref, wi1_ref, wf_ref, go_hbm,
                 y_hbm, small_ref, dq_ref, dk_ref, dv_ref, do_ref, di0_ref, di1_ref, df_ref,
                 tab_s, pad_s, ga_s, gm_s, wqkv_s, wo_s, wi_s, wf_s, wqkvt_s, wot_s, wit_s, wft_s, xt_s, qkv_s, p_s, ctx_s,
                 got_s, ut_s, zt_s, dgu_s, dh_s, dga_s, dgm_s, io_s, idx_s,
                 *more):
    (acc, rd, r1, r2, rz, out), more = [more[i * NG:(i + 1) * NG] for i in range(6)], more[6 * NG:]
    sm_s, smr_s, smz_s, io_sem, out_sem, ag_own, ag_send, ag_recv, rs_send, rs_recv = more
    at = Place()
    barrier = pltpu.get_barrier_semaphore()
    peers = [at.sib, at.nx, at.ny, at.nd] + at.nz
    for dev in peers:
        pl.semaphore_signal(barrier, inc=1, device_id=dev, device_id_type=MESH)

    def rows_of(r):
        return pl.ds(pl.multiple_of(r * SEQ, SEQ), SEQ)

    def x_copy(r):
        return pltpu.make_async_copy(x_hbm.at[rows_of(r), :], io_s.at[rows_of(r), :], io_sem.at[0, r])

    def go_copy(r):
        return pltpu.make_async_copy(go_hbm.at[rows_of(r), :], io_s.at[rows_of(r), :], io_sem.at[1, r])

    def y_copy(r):
        return pltpu.make_async_copy(io_s.at[rows_of(r), :], y_hbm.at[rows_of(r), :], io_sem.at[2, r])

    gather = Gather(at, (wq_ref, wk_ref, wv_ref, wo_ref, wi0_ref, wi1_ref, wf_ref),
                    ((wqkv_s, 0), (wqkv_s, AW), (wqkv_s, 2 * AW), (wo_s, 0), (wi_s, 0), (wi_s, FF), (wf_s, 0)), ag_own, ag_send, ag_recv)
    for w in range(7):
        gather.load(w).start()
    for r in range(ROWS):
        x_copy(r).start()
    pl.semaphore_wait(barrier, len(peers))
    first, rest = (0, 1, 2), (3, 4, 5, 6)
    gather.begin(first, (2, 0, 1, 3))
    gather.begin(rest, (0, 1, 3))
    setup_small(relb_ref, ga_ref, gm_ref, tab_s, pad_s, ga_s, gm_s)
    dgm_s[...] = jnp.zeros_like(dgm_s)
    dga_s[...] = jnp.zeros_like(dga_s)

    def prep(r):
        x_copy(r).wait()
        prep_row(r, io_s, pos_ref, seg_ref, ga_s, xt_s, ut_s, idx_s)
        go_copy(r).start()
    loop(ROWS, prep)

    def prep_go(r):
        go_copy(r).wait()
        got_s[:, tok_slice(r)] = io_s[tok_slice(r), :].T
    loop(ROWS, prep_go)
    gather.relay(first)
    gather.finish(first)
    wqkvt_s[...] = wqkv_s[...].T
    loop(TOK // 512, lambda r: qkv_block(r, wqkvt_s, ut_s, qkv_s))

    def fwd(r):
        attn_fwd_row(r, tab_s, idx_s, qkv_s, p_s, ctx_s)

        @pl.when(r == 0)
        def _():
            gather.relay1((3, 4))

        @pl.when(r == 2)
        def _():
            gather.relay1((5,))

        @pl.when(r == 3)
        def _():
            gather.relay1((6,))
            gather.relay2((3, 4))
    loop(ROWS, fwd)
    gather.relay2((5, 6))
    gather.finish((3, 4))
    wot_s[...] = wo_s[...].T
    wit_s[0:FF, :] = wi_s[:, 0:FF].T
    gather.finish((5, 6))
    wit_s[FF:2 * FF, :] = wi_s[:, FF:2 * FF].T
    wft_s[...] = wf_s[...].T

    mlp_in_row(0, gm_s, wot_s, xt_s, ctx_s, ut_s, dh_s)

    def mlp_up(r):
        mlp_up_row(r, gm_s, wot_s, wit_s, wf_s, xt_s, ctx_s, got_s, ut_s, zt_s, dgu_s, dh_s)
    loop(ROWS, mlp_up)

    red = [Reduce(a, at, acc[a], rd[a], r1[a], r2[a], rz[a], out[a], rs_send, rs_recv) for a in range(NG)]
    small = Small(at, sm_s, smr_s, smz_s, rs_send, rs_recv)

    def cols(c, n=256):
        return pl.ds(pl.multiple_of(c * n, n), n)

    def fire(name, i):
        for step, g in PLAN.get((name, i), ()):
            {'d': red[g].d_send, 'a': red[g].xy1, 'b': red[g].xy2, 'y': red[g].z1, 'z': red[g].z2}[step]()

    def fire_at(name, i, n, base=0):
        for k in range(base, base + n):
            if (name, k) in PLAN:
                pl.when(i == k)(functools.partial(fire, name, k))

    for i in range(2):
        acc[i][...] = mm_nt(zt_s[...], got_s[256 * i:256 * i + 256, :])
        fire('wf', i)
    for g in range(4):
        def dwi(c, g=g):
            acc[2 + g][:, cols(c)] = mm_nt(ut_s[...], dgu_s[cols(c + 2 * g), :])
            fire_at('wi', c + 2 * g, 2, 2 * g)
        loop(2, dwi)

    def mlp_down(r):
        mlp_down_row(r, io_s, gm_s, wft_s, wi_s, got_s, zt_s, dgu_s, dh_s, dgm_s)
        y_copy(r).start()
        fire_at('down', r, ROWS)
    loop(ROWS, mlp_down)

    def dwo(c):
        acc[6][:, cols(c)] = mm_nt(ctx_s[...], dh_s[cols(c), :])
    loop(2, dwo)
    fire('wo', 0)

    def bwd(r):
        attn_bwd_row(r, ga_s, wo_s, xt_s, ut_s, qkv_s, p_s, dh_s, dgu_s)
        fire_at('bwd', r, ROWS)
    loop(ROWS, bwd)
    for i in range(3):
        acc[7 + i][...] = mm_nt(ut_s[...], dgu_s[AW * i:AW * i + AW, :])
        fire('wqkv', i)

    for g in range(2):
        red[g].drain()
        acc[g][...] = jnp.zeros_like(acc[g])

    def tail(r):
        bias_row(r, pos_ref, p_s, acc)
        gain_row(r, wqkv_s, xt_s, dgu_s, dga_s)
        fire_at('tail', r, ROWS)
    loop(ROWS, tail)
    db_s = p_s.at[0, 0]
    db_s[...] = jnp.zeros_like(db_s)
    bias_sums(acc, db_s)
    sm_s[0, 0:1, 0:256] = jnp.sum(p_s[0, 0].T, axis=0, keepdims=True)
    sm_s[0, 0:1, 256:512] = jnp.zeros((1, 256), F32)
    sm_s[0, 1:2, :] = jnp.sum(dga_s[...].T, axis=0, keepdims=True)
    sm_s[0, 2:3, :] = jnp.sum(dgm_s[...].T, axis=0, keepdims=True)
    sm_s[0, 3:8, :] = jnp.zeros((5, 512), F32)
    small.advance(0)
    fire('head', 0)
    small.advance(1)
    late = PLAN.get(('end', 0), ())
    finals = [(df_ref, 0, 256), (df_ref, 256, 256), (di0_ref, 0, 512), (di0_ref, 512, 512), (di1_ref, 0, 512), (di1_ref, 512, 512),
              (do_ref, 0, 512), (dq_ref, 0, AW), (dk_ref, 0, AW), (dv_ref, 0, AW)]
    finals = [pltpu.make_async_copy(out[g], dst.at[:, pl.ds(c, n)], out_sem.at[g]) for g, (dst, c, n) in enumerate(finals)]
    held = [g for _, g in late]
    for step, g in late[:1]:
        red[g].z2()
    small.advance(2)
    for step, g in late[1:]:
        red[g].z2()
    small.advance(3)
    for g in [g for g in range(NG) if g not in held] + held:
        red[g].finish()
        finals[g].start()
    small_ref[...] = small.finish()
    for copy in finals:
        copy.wait()
    for r in range(ROWS):
        y_copy(r).wait()
    gather.drain(first, False)
    gather.drain(rest, True)
    for g in red[2:]:
        g.drain()
    small.drain()


def emit_kernel(y_in, small_ref, g0, g1, g2, g3, g4, g5, g6, y_out, db_ref, dga_ref, dgm_ref, o0, o1, o2, o3, o4, o5, o6,
                y_s, b0, b1, b2, b3, b4, b5, b6, in_sem, out_sem):
    pairs = [(y_in.at[pl.ds(r * SEQ, SEQ), :], y_s.at[pl.ds(r * SEQ, SEQ), :], y_out.at[pl.ds(r * SEQ, SEQ), :]) for r in range(ROWS)]
    pairs += list(zip((g0, g1, g2, g3, g4, g5, g6), (b0, b1, b2, b3, b4, b5, b6), (o0, o1, o2, o3, o4, o5, o6)))
    ins = [pltpu.make_async_copy(a, b, in_sem.at[i]) for i, (a, b, _) in enumerate(pairs)]
    outs = [pltpu.make_async_copy(b, c, out_sem.at[i]) for i, (_, b, c) in enumerate(pairs)]
    for copy in ins:
        copy.start()
    for h in range(HEADS):
        db_ref[h:h + 1, :] = small_ref[0:1, h * 32:(h + 1) * 32]
    dga_ref[...] = small_ref[1:2, :]
    dgm_ref[...] = small_ref[2:3, :]
    for i in range(len(pairs)):
        ins[i].wait()
        outs[i].start()
    for copy in outs:
        copy.wait()


def local_layer(x_in, positions, segments, rel_bias, gain_attn, gain_mlp, wq, wk, wv, wo, wi0, wi1, wf, grad_out):
    vmem = pl.BlockSpec(memory_space=pltpu.VMEM)
    hbm = pl.BlockSpec(memory_space=pl.ANY)

    def bufs(shape_of, dtype):
        return [pltpu.VMEM(shape_of(r, c), dtype) for r, c in SHARD]

    def quarter(r, c):
        return (3, r, 128) if r == 48 else (3, r // 4, c)
    outs = pl.pallas_call(
        layer_kernel,
        out_shape=[jax.ShapeDtypeStruct((TOK, DM), BF16), jax.ShapeDtypeStruct((8, 512), F32)]
        + [jax.ShapeDtypeStruct(w.shape, BF16) for w in (wq, wk, wv, wo, wi0, wi1, wf)],
        in_specs=[hbm] + [vmem] * 5 + [hbm] * 8,
        out_specs=[hbm, vmem] + [hbm] * 7,
        scratch_shapes=[
            pltpu.VMEM((8, 128), F32), pltpu.VMEM((128, 128), F32), pltpu.VMEM((DM, 128), F32), pltpu.VMEM((DM, 128), F32),
            pltpu.VMEM((DM, 3 * AW), BF16), pltpu.VMEM((AW, DM), BF16), pltpu.VMEM((DM, 2 * FF), BF16), pltpu.VMEM((FF, DM), BF16),
            pltpu.VMEM((3 * AW, DM), BF16), pltpu.VMEM((DM, AW), BF16), pltpu.VMEM((2 * FF, DM), BF16), pltpu.VMEM((DM, FF), BF16),
            pltpu.VMEM((DM, TOK), BF16), pltpu.VMEM((3 * AW, TOK), BF16),
            pltpu.VMEM((HEADS, ROWS, SEQ, SEQ), F32), pltpu.VMEM((AW, TOK), BF16),
            pltpu.VMEM((DM, TOK), BF16), pltpu.VMEM((DM, TOK), BF16), pltpu.VMEM((FF, TOK), BF16), pltpu.VMEM((2 * FF, TOK), BF16),
            pltpu.VMEM((DM, TOK), BF16), pltpu.VMEM((DM, 128), F32), pltpu.VMEM((DM, 128), F32),
            pltpu.VMEM((TOK, DM), BF16), pltpu.VMEM((ROWS, SEQ, SEQ), jnp.int32)]
        + bufs(lambda r, c: (8 * r, c), F32) + bufs(lambda r, c: (4, r, c), F32) + bufs(lambda r, c: (4, r // 2, c), F32)
        + bufs(lambda r, c: (2, r // 2, c), F32) + bufs(quarter, F32) + bufs(lambda r, c: (r, c), BF16)
        + [pltpu.VMEM((3, 8, 512), F32), pltpu.VMEM((3, 8, 512), F32), pltpu.VMEM((4, 8, 512), F32),
           pltpu.SemaphoreType.DMA((3, ROWS)), pltpu.SemaphoreType.DMA((NG,)), pltpu.SemaphoreType.DMA((7,)), pltpu.SemaphoreType.DMA((63,)), pltpu.SemaphoreType.DMA((63,)),
           pltpu.SemaphoreType.DMA((NG * NSEM + 6,)), pltpu.SemaphoreType.DMA((NG * NSEM + 6,))],
        compiler_params=pltpu.CompilerParams(vmem_limit_bytes=67043328, collective_id=0, has_side_effects=True),
        name='layer',
    )(x_in.reshape(TOK, DM), positions, segments, rel_bias.T,
      gain_attn.reshape(1, DM), gain_mlp.reshape(1, DM), wq, wk, wv, wo, wi0, wi1, wf, grad_out.reshape(TOK, DM))
    weights = (wq, wk, wv, wo, wi0, wi1, wf)
    outs = pl.pallas_call(
        emit_kernel,
        out_shape=[jax.ShapeDtypeStruct((TOK, DM), BF16), jax.ShapeDtypeStruct((HEADS, 32), F32),
                   jax.ShapeDtypeStruct((1, DM), F32), jax.ShapeDtypeStruct((1, DM), F32)]
        + [jax.ShapeDtypeStruct(w.shape, BF16) for w in weights],
        in_specs=[hbm, vmem] + [hbm] * 7,
        out_specs=[hbm, vmem, vmem, vmem] + [hbm] * 7,
        scratch_shapes=[pltpu.VMEM((TOK, DM), BF16)] + [pltpu.VMEM(w.shape, BF16) for w in weights]
        + [pltpu.SemaphoreType.DMA((ROWS + 7,)), pltpu.SemaphoreType.DMA((ROWS + 7,))],
        name='emit',
    )(*outs)
    y, db, dga, dgm = outs[:4]
    return (y.reshape(ROWS, SEQ, DM), db.T, dga.reshape(DM), dgm.reshape(DM)) + tuple(outs[4:])


def solution(mesh):
    row_spec = P(ROW_AXES)
    whole = P()
    part_spec = P('fsdp')
    in_specs = (row_spec, row_spec, row_spec, whole, whole, whole) + (part_spec,) * 7 + (row_spec,)
    out_specs = (row_spec, whole, whole, whole) + (part_spec,) * 7
    return jax.shard_map(local_layer, mesh=mesh, in_specs=in_specs, out_specs=out_specs, check_vma=False)
```

```python
import functools
import jax
import jax.numpy as jnp
from jax import lax
from jax.experimental import pallas as pl
from jax.experimental.pallas import tpu as pltpu
from jax.sharding import PartitionSpec as P
ZERO, ONE, TWO = (0, 1, 2)
EPSILON = 1e-06
NEG_BIG = -1000000000.0
THRESHOLDS = (12, 16, 23, 32, 46, 64, 91)
ROW_AXES = ('dp', 'fsdp')
ROWS, SEQ, DM, HEADS, HD, FF = (6, 256, 512, 6, 64, 1024)
TOK = ROWS * SEQ
EARLY = 4
AW = HEADS * HD
F32, BF16 = (jnp.float32, jnp.bfloat16)

def mm(a, b):
    return lax.dot_general(a, b, (((ONE,), (ZERO,)), ((), ())), preferred_element_type=F32)

def mm_nt(a, b):
    return lax.dot_general(a, b, (((ONE,), (ONE,)), ((), ())), preferred_element_type=F32)

def mm_tn(a, b):
    return lax.dot_general(a, b, (((ZERO,), (ZERO,)), ((), ())), preferred_element_type=F32)

def split3(v):
    hi = v.astype(BF16)
    rest = v - hi.astype(F32)
    mid = rest.astype(BF16)
    lo = (rest - mid.astype(F32)).astype(BF16)
    return (hi, mid, lo)

def tok_slice(r):
    return pl.ds(pl.multiple_of(r * SEQ, SEQ), SEQ)

def rel_class(diff):
    m = jnp.abs(diff)
    e = jnp.minimum(m, 8.0)
    for bound in THRESHOLDS:
        e = e + jnp.where(m >= bound, 1.0, 0.0)
    return e + jnp.where(diff > ZERO, 16.0, 0.0)

def setup_small(relb_ref, ga_ref, gm_ref, tab_s, pad_s, ga_s, gm_s):
    pad_s[...] = jnp.zeros_like(pad_s)
    pad_s[ZERO:HEADS, ZERO:32] = relb_ref[...]
    t = pad_s[ZERO:8, :]
    lane = lax.broadcasted_iota(jnp.int32, t.shape, ONE)
    tab_s[...] = jnp.where(lane < 32, t, pltpu.roll(t, 32, ONE) + NEG_BIG)
    ga_s[...] = jnp.broadcast_to(ga_ref[...], (128, DM)).T
    gm_s[...] = jnp.broadcast_to(gm_ref[...], (128, DM)).T

def wide(col128):
    return jnp.concatenate([col128, col128], axis=ONE)

def prep_row(r, x_ref, ga_s, xt_s, at_s):
    tok = tok_slice(r)
    xt = x_ref[tok, :].T
    xt_s[:, tok] = xt
    xf = xt.astype(F32)
    inv = lax.rsqrt(jnp.mean(xf * xf, axis=ZERO, keepdims=True) + EPSILON)
    at_s[:, tok] = (xf * inv * wide(ga_s[...])).astype(BF16)

def table_row(r, pos_ref, seg_ref, tab_s, idx_s, p_s):
    code = (seg_ref[pl.ds(r, ONE), :] * 1024 + pos_ref[pl.ds(r, ONE), :]).astype(F32)
    code = jnp.broadcast_to(code, (SEQ, SEQ))
    diff = code.T - code
    idx = (rel_class(diff) + jnp.where(jnp.abs(diff) >= 512.0, 32.0, 0.0)).astype(jnp.int32)
    idx_s[r] = idx
    for h in range(EARLY):
        table = jnp.broadcast_to(tab_s[h:h + ONE, :], (SEQ, 128))
        p_s[h, r, :, ZERO:128] = lane_lookup(table, idx[:, ZERO:128])
        p_s[h, r, :, 128:256] = lane_lookup(table, idx[:, 128:256])

def lane_lookup(table, idx):
    dims = lax.GatherDimensionNumbers(offset_dims=(), collapsed_slice_dims=(ONE,), start_index_map=(ONE,), operand_batching_dims=(ZERO,), start_indices_batching_dims=(ZERO,))
    return lax.gather(table, idx[:, :, None], dims, (ONE, ONE), mode='promise_in_bounds')

def qkv_block(r, wqkvt_s, at_s, qkv_s):
    tok = pl.ds(pl.multiple_of(r * 512, 512), 512)
    qkv_s[:, tok] = mm(wqkvt_s[...], at_s[:, tok]).astype(BF16)

def attn_fwd_row(r, tab_s, idx_s, qkv_s, p_s, ctx_s):
    tok = tok_slice(r)
    half = SEQ // TWO

    def scores(h):
        kt, qt = (qkv_s[AW + h * HD:AW + (h + ONE) * HD, tok], qkv_s[h * HD:(h + ONE) * HD, tok])
        return [mm_tn(kt, qt[:, ZERO:half]), mm_tn(kt, qt[:, half:SEQ])]
    ahead = [scores(h) for h in range(TWO)]
    for h in range(HEADS):
        s_now = ahead.pop(ZERO)
        if h + TWO < HEADS:
            ahead.append(scores(h + TWO))
        low = []
        for i in range(TWO):
            cols = slice(i * half, (i + ONE) * half)
            bias = p_s[h, r, :, cols] if h < EARLY else lane_lookup(jnp.broadcast_to(tab_s[h:h + ONE, :], (SEQ, 128)), idx_s[r, :, cols])
            s = s_now[i] + bias
            p = jnp.exp(s - jnp.max(s, axis=ZERO, keepdims=True))
            p = p * (1.0 / jnp.sum(p, axis=ZERO, keepdims=True))
            p_s[h, r, :, cols] = p
            low.append(p.astype(BF16))
        vt = qkv_s[TWO * AW + h * HD:TWO * AW + (h + ONE) * HD, tok]
        ctx_s[h * HD:(h + ONE) * HD, tok] = mm(vt, jnp.concatenate(low, axis=ONE)).astype(BF16)

def mlp_in_row(r, gm_s, wot_s, xt_s, ctx_s, ut_s, h_s):
    tok = tok_slice(r)
    ht = (xt_s[:, tok].astype(F32) + mm(wot_s[...], ctx_s[:, tok])).astype(BF16)
    h_s[:, tok] = ht
    hf = ht.astype(F32)
    inv = lax.rsqrt(jnp.mean(hf * hf, axis=ZERO, keepdims=True) + EPSILON)
    ut_s[:, tok] = (hf * inv * wide(gm_s[...])).astype(BF16)

def mlp_up_row(r, gm_s, wot_s, wit_s, wf_s, xt_s, ctx_s, got_s, ut_s, zt_s, dgu_s, h_s):
    tok = tok_slice(r)
    ut, got = (ut_s[:, tok], got_s[:, tok])
    step = 256

    def products(f):
        return (mm(wit_s[f:f + step, :], ut), mm(wit_s[FF + f:FF + f + step, :], ut), mm(wf_s[f:f + step, :], got))
    nxt = products(ZERO)
    mlp_in_row(jnp.minimum(r + ONE, ROWS - ONE), gm_s, wot_s, xt_s, ctx_s, ut_s, h_s)
    for f in range(ZERO, FF, step):
        gate, up, dz = nxt
        if f + step < FF:
            nxt = products(f + step)
        dz = dz.astype(BF16).astype(F32)
        sg = 1.0 / (1.0 + jnp.exp(-gate))
        silu = gate * sg
        zt_s[f:f + step, tok] = (silu * up).astype(BF16)
        dgu_s[f:f + step, tok] = (dz * up * (sg * (1.0 + gate * (1.0 - sg)))).astype(BF16)
        dgu_s[FF + f:FF + f + step, tok] = (dz * silu).astype(BF16)

def mlp_down_row(r, gm_s, wi_s, got_s, dgu_s, h_s, dgm_s):
    tok = tok_slice(r)
    ht, got = (h_s[:, tok], got_s[:, tok])
    hf = ht.astype(F32)
    inv = lax.rsqrt(jnp.mean(hf * hf, axis=ZERO, keepdims=True) + EPSILON)
    gm = wide(gm_s[...])
    du = mm(wi_s[...], dgu_s[:, tok]).astype(BF16).astype(F32)
    hn = hf * inv
    dg = du * hn
    dgm_s[...] += dg[:, ZERO:128] + dg[:, 128:256]
    dug = du * gm
    dhn = inv * (dug - hn * jnp.mean(dug * hn, axis=ZERO, keepdims=True))
    h_s[:, tok] = (got.astype(F32) + dhn).astype(BF16)
    got_s[:, tok] = ht

def out_row(r, y_ref, wft_s, h_s, zt_s):
    tok = tok_slice(r)
    y_ref[tok, :] = (h_s[:, tok].astype(F32) + mm(wft_s[...], zt_s[:, tok])).astype(BF16).T

def attn_bwd_row(r, ga_s, wo_s, xt_s, at_s, qkv_s, p_s, dh_s, dqkv_s):
    tok = tok_slice(r)
    dct = mm(wo_s[...], dh_s[:, tok]).astype(BF16)
    qkv = qkv_s[:, tok]

    def dprob(h):
        return mm_tn(qkv[TWO * AW + h * HD:TWO * AW + (h + ONE) * HD], dct[h * HD:(h + ONE) * HD])
    ahead = [dprob(h) for h in range(TWO)]
    for h in range(HEADS):
        dp = ahead.pop(ZERO)
        if h + TWO < HEADS:
            ahead.append(dprob(h + TWO))
        p = p_s[h, r]
        dqkv_s[TWO * AW + h * HD:TWO * AW + (h + ONE) * HD, tok] = mm_nt(dct[h * HD:(h + ONE) * HD], p.astype(BF16)).astype(BF16)
        ds = p * (dp - jnp.sum(dp * p, axis=ZERO, keepdims=True))
        p_s[h, r] = ds
        low = ds.astype(BF16)
        dqkv_s[h * HD:(h + ONE) * HD, tok] = mm(qkv[AW + h * HD:AW + (h + ONE) * HD], low).astype(BF16)
        dqkv_s[AW + h * HD:AW + (h + ONE) * HD, tok] = mm_nt(qkv[h * HD:(h + ONE) * HD], low).astype(BF16)
    xf = xt_s[:, tok].astype(F32)
    inv = lax.rsqrt(jnp.mean(xf * xf, axis=ZERO, keepdims=True) + EPSILON)
    at_s[:, tok] = (xf * inv * wide(ga_s[...])).astype(BF16)

def bias_view(dacc, h):
    return dacc[h // 4].at[h % 4 * SEQ:(h % 4 + ONE) * SEQ, :]

def bias_row(r, pos_ref, p_s, dacc):
    pos = pos_ref[pl.ds(r, ONE), :]
    onehot = jnp.where(lax.broadcasted_iota(jnp.int32, (SEQ, SEQ), ZERO) == pos, 1.0, 0.0).astype(BF16)

    def first(h):
        hi, mid, lo = split3(p_s[h, r])
        return mm(onehot, hi) + mm(onehot, mid) + mm(onehot, lo)
    nxt = first(ZERO)
    for h in range(HEADS):
        t = nxt
        if h + ONE < HEADS:
            nxt = first(h + ONE)
        hi, mid, lo = split3(t)
        bias_view(dacc, h)[...] += mm_nt(hi, onehot) + mm_nt(mid, onehot) + mm_nt(lo, onehot)

def gain_row(r, wqkv_s, xt_s, dqkv_s, dga_s):
    tok = tok_slice(r)
    dn = mm(wqkv_s[...], dqkv_s[ZERO:3 * AW, tok]).astype(BF16).astype(F32)
    xf = xt_s[:, tok].astype(F32)
    inv = lax.rsqrt(jnp.mean(xf * xf, axis=ZERO, keepdims=True) + EPSILON)
    dg = dn * (xf * inv)
    dga_s[...] += dg[:, ZERO:128] + dg[:, 128:256]

def bias_sums(dacc, db_s):
    sub = lax.broadcasted_iota(jnp.int32, (8, SEQ), ZERO)
    lane = lax.broadcasted_iota(jnp.int32, (8, SEQ), ONE)
    below = (sub - lane).astype(F32)
    above = jnp.where(lane <= sub, sub - lane, sub - lane + SEQ).astype(F32)
    cls_a, cls_b = (rel_class(above), rel_class(below))

    def head(h, src, first):
        acc_a = jnp.zeros((8, SEQ), F32)
        acc_b = jnp.zeros((8, SEQ), F32)
        for t in range(SEQ // 8):
            d = src[pl.ds(pl.multiple_of(h * SEQ + 8 * t, 8), 8), :]
            keep = lane <= sub + 8 * t
            a, b = (jnp.where(keep, d, 0.0), jnp.where(keep, 0.0, d))
            if t > ZERO:
                a, b = (pltpu.roll(a, SEQ - 8 * t, ONE), pltpu.roll(b, SEQ - 8 * t, ONE))
            acc_a, acc_b = (acc_a + a, acc_b + b)
        for c in range(32):
            if c < 16:
                v = jnp.where(cls_b == float(c), acc_b, 0.0)
                if c == ZERO:
                    v = v + jnp.where(cls_a == 0.0, acc_a, 0.0)
            else:
                v = jnp.where(cls_a == float(c), acc_a, 0.0)
            db_s[pl.ds((h + first) * 32 + c, ONE), :] = jnp.sum(v, axis=ZERO, keepdims=True)
    loop(4, lambda h: head(h, dacc[ZERO], ZERO))
    loop(HEADS - 4, lambda h: head(h, dacc[ONE], 4))

def loop(n, fn):

    def body(i, carry):
        fn(i)
        return carry
    lax.fori_loop(ZERO, n, body, ZERO)
MESH = pl.DeviceIdType.MESH
SHARD = ((128, 256),) * 2 + ((64, 512),) * 4 + ((48, 512),) + ((64, 384),) * 3
NG = len(SHARD)
PAIRED = (0, 1, 2, 3, 4, 5, 6)
PLAN = {'wf0': 'd0', 'wf1': 'd1', 'wi0': 'a0', 'wi1': 'd2', 'wi2': 'a1', 'wi3': 'd3', 'wi5': 'd4', 'wi7': 'd5a4', 'down2': 'b1a2', 'down5': 'b0b4', 'wo0': 'd6y1', 'bwd0': 'a6', 'bwd1': 'b2w1', 'bwd2': 'y0', 'bwd3': 'a3y4', 'bwd4': 'a5w0z1', 'bwd5': 'y2w4', 'wqkv0': 'd7b6', 'wqkv1': 'd8b3a7x1', 'wqkv2': 'd9w2z0', 'tail0': 'b5z4', 'gain0': 'y6', 'tail1': 'y3z2', 'gain1': 'x0', 'tail2': 'b7w6', 'gain2': 'a8w3y5', 'tail3': 'a9y7x2', 'gain3': 'z6', 'tail4': 'b8w5', 'gain4': 'b9x4', 'tail5': 'z3y8', 'gain5': 'x6z7z5', 'head0': 'y9', 'yrow2': 'x3', 'yrow3': 'z8', 'yrow5': 'z9', 'yrow4': 'x5'}
NSEM = 16

def remote(src, dst, send, recv, i, dev):
    return pltpu.make_async_remote_copy(src_ref=src, dst_ref=dst, send_sem=send.at[i], recv_sem=recv.at[i], device_id=dev, device_id_type=MESH)

class Place:

    def __init__(self):
        self.f = lax.axis_index('fsdp')
        self.z = lax.axis_index('dp')
        self.c = lax.rem(self.f, TWO)
        self.k = self.f // TWO
        self.x = lax.rem(self.k, TWO)
        self.y = self.k // TWO
        self.kx = self.k + ONE - TWO * self.x
        self.ky = self.k + TWO - 4 * self.y
        self.kd = 3 - self.k
        self.sib = {'fsdp': self.f + ONE - TWO * self.c}
        self.nx = {'fsdp': TWO * self.kx + self.c}
        self.ny = {'fsdp': TWO * self.ky + self.c}
        self.nd = {'fsdp': TWO * self.kd + self.c}
        self.up = [lax.rem(self.z + j, 4) for j in (ONE, TWO, 3)]
        self.nz = [{'dp': u} for u in self.up]
        self.za = lax.rem(self.z, TWO)
        self.zb = self.z // TWO
        self.n1 = {'dp': self.z + ONE - TWO * self.za}
        self.n2 = {'dp': self.z + TWO - 4 * self.zb}

class Gather:
    N = 9

    def __init__(self, at, parts, fulls, own, send, recv):
        self.at, self.parts, self.fulls, self.own, self.send, self.recv = (at, parts, fulls, own, send, recv)

    def view(self, w, f, h=None):
        full, col = self.fulls[w]
        rows, cols = self.parts[w].shape
        off = f * rows
        if h is not None:
            cut = (rows // TWO + 15) // 16 * 16
            off = off + h * cut
            rows = cut if h == ZERO else rows - cut
        return full.at[pl.ds(pl.multiple_of(off, 16), rows), pl.ds(col, cols)]

    def load(self, w):
        return pltpu.make_async_copy(self.parts[w], self.view(w, self.at.f), self.own.at[w])

    def direct(self, w, j):
        at = self.at
        v = self.view(w, at.f)
        return remote(v, v, self.send, self.recv, w * self.N + j, (at.nx, at.ny, at.nd, at.sib)[j])

    def forward(self, w, j):
        at = self.at
        v = self.view(w, TWO * (at.kx, at.ky, at.kd)[j] + at.c)
        return remote(v, v, self.send, self.recv, w * self.N + 4 + j, at.sib)

    def diag(self, w, h):
        at = self.at
        v = self.view(w, TWO * (at.kx, at.ky)[h] + at.c, h)
        return remote(v, v, self.send, self.recv, w * self.N + 7 + h, (at.ny, at.nx)[h])

    def begin(self, ws, js):
        for w in ws:
            self.load(w).wait()
            for j in js:
                self.direct(w, j).start()

    def relay(self, ws):
        for w in ws:
            for j in (ZERO, ONE, TWO):
                self.direct(w, j).wait_recv()
                self.forward(w, j).start()

    def relay1(self, ws):
        for w in ws:
            for j in (ZERO, ONE):
                self.direct(w, j).wait_recv()
                self.diag(w, j).start()
                self.forward(w, j).start()

    def relay2(self, ws):
        for w in ws:
            self.diag(w, ZERO).wait_recv()
            self.diag(w, ONE).wait_recv()
            self.forward(w, TWO).start()

    def finish(self, ws):
        for w in ws:
            self.direct(w, 3).wait_recv()
            for j in (ZERO, ONE, TWO):
                self.forward(w, j).wait_recv()

    def drain(self, ws, halves):
        for w in ws:
            for j in (ZERO, ONE, 3) if halves else (ZERO, ONE, TWO, 3):
                self.direct(w, j).wait_send()
            for j in range(3):
                self.forward(w, j).wait_send()
            if halves:
                self.diag(w, ZERO).wait_send()
                self.diag(w, ONE).wait_send()

class Reduce:

    def __init__(self, a, at, acc, rd, r1, r2, rz, out, send, recv):
        self.a, self.at, self.acc, self.rd, self.r1, self.r2, self.rz, self.out = (a, at, acc, rd, r1, r2, rz, out)
        self.send, self.recv = (send, recv)
        self.rows, self.cols = SHARD[a]
        self.half = self.rows // TWO

    def part(self, k, c, h=None):
        n = self.rows if h is None else self.half
        off = (TWO * k + c) * self.rows + (ZERO if h is None else h * self.half)
        return self.acc.at[pl.ds(pl.multiple_of(off, 8), n), :]

    def copy(self, src, dst, i, dev):
        return remote(src, dst, self.send, self.recv, self.a * NSEM + i, dev)

    def d_copy(self, i):
        at = self.at
        k = (at.kd, at.kx, at.ky, at.k)[i]
        return self.copy(self.part(k, ONE - at.c), self.rd.at[i], i, at.sib)

    def xy1_copy(self, i):
        at = self.at
        k, h, dev = ((at.kx, ZERO, at.nx), (at.kd, ZERO, at.nx), (at.ky, ONE, at.ny), (at.kd, ONE, at.ny))[i]
        return self.copy(self.part(k, at.c, h), self.r1.at[i], 4 + i, dev)

    def xy2_copy(self, i):
        at = self.at
        k, h, dev = ((at.ky, ZERO, at.ny), (at.kx, ONE, at.nx))[i]
        return self.copy(self.part(k, at.c, h), self.r2.at[i], 8 + i, dev)

    def quarter(self, z, base):
        if self.rows == 48:
            return (pl.ds(base, self.rows), pl.ds(pl.multiple_of(z * 128, 128), 128))
        n = self.rows // 4
        return (pl.ds(pl.multiple_of(base + z * n, 16), n), slice(None))

    def z1_copy(self, j):
        at = self.at
        rows, cols = self.quarter(at.up[j], pl.multiple_of(at.f * self.rows, 16))
        return self.copy(self.acc.at[rows, cols], self.rz.at[j], 10 + j, at.nz[j])

    def z2_copy(self, j):
        at = self.at
        rows, cols = self.quarter(at.z, ZERO)
        v = self.out.at[rows, cols]
        return self.copy(v, v, 13 + j, at.nz[j])

    def d_send(self):
        for i in range(4):
            self.d_copy(i).start()

    def add(self, view, buf):
        view[...] = view[...] + buf[...]

    def xy1(self):
        at = self.at
        for i, k in enumerate((at.kd, at.kx, at.ky, at.k)):
            self.d_copy(i).wait_recv()
            self.add(self.part(k, at.c), self.rd.at[i])
        for i in (ZERO, TWO, ONE, 3):
            self.xy1_copy(i).start()

    def xy2(self):
        at = self.at
        for i, (k, h) in ((ONE, (at.ky, ZERO)), (3, (at.kx, ONE)), (ZERO, (at.k, ZERO)), (TWO, (at.k, ONE))):
            self.xy1_copy(i).wait_recv()
            self.add(self.part(k, at.c, h), self.r1.at[i])
            if i == ONE:
                self.xy2_copy(ZERO).start()
            if i == 3:
                self.xy2_copy(ONE).start()

    def z1(self):
        at = self.at
        for i in range(TWO):
            self.xy2_copy(i).wait_recv()
            self.add(self.part(at.k, at.c, i), self.r2.at[i])
        for j in (ONE, ZERO, TWO):
            self.z1_copy(j).start()

    def z2(self):
        at = self.at
        rows, cols = self.quarter(at.z, pl.multiple_of(at.f * self.rows, 16))
        total = self.acc[rows, cols]
        for j in range(3):
            self.z1_copy(j).wait_recv()
            total = total + self.rz[j]
        rows, cols = self.quarter(at.z, ZERO)
        self.out[rows, cols] = total.astype(BF16)
        for j in (ONE, ZERO, TWO):
            self.z2_copy(j).start()

    def finish(self):
        for j in range(3):
            self.z2_copy(j).wait_recv()

    def drain(self):
        for i in range(4):
            self.d_copy(i).wait_send()
            self.xy1_copy(i).wait_send()
        for i in range(TWO):
            self.xy2_copy(i).wait_send()
        for i in range(3):
            self.z1_copy(i).wait_send()
            self.z2_copy(i).wait_send()

class Paired(Reduce):

    def piece(self, base, i, n):
        if self.rows == 48:
            return (pl.ds(pl.multiple_of(base, 16), self.rows), pl.ds(pl.multiple_of(i * 128, 128), n * 128))
        q = self.rows // 4
        return (pl.ds(pl.multiple_of(base + i * q, 16), n * q), slice(None))

    def y_copy(self):
        at = self.at
        rows, cols = self.piece(at.f * self.rows, TWO * (ONE - at.za), TWO)
        return self.copy(self.acc.at[rows, cols], self.rz[ZERO], 10, at.n1)

    def w_copy(self):
        at = self.at
        rows, cols = self.piece(at.f * self.rows, TWO * at.za + ONE - at.zb, ONE)
        return self.copy(self.acc.at[rows, cols], self.rz[ONE], 11, at.n2)

    def z_copy(self):
        at = self.at
        rows, cols = self.piece(ZERO, TWO * at.za + at.zb, ONE)
        v = self.out.at[rows, cols]
        return self.copy(v, v, 12, at.n2)

    def x_copy(self):
        at = self.at
        rows, cols = self.piece(ZERO, TWO * at.za, TWO)
        v = self.out.at[rows, cols]
        return self.copy(v, v, 13, at.n1)

    def z1(self):
        at = self.at
        for i in range(TWO):
            self.xy2_copy(i).wait_recv()
            self.add(self.part(at.k, at.c, i), self.r2.at[i])
        self.y_copy().start()

    def w1(self):
        at = self.at
        self.y_copy().wait_recv()
        rows, cols = self.piece(at.f * self.rows, TWO * at.za, TWO)
        self.add(self.acc.at[rows, cols], self.rz[ZERO])
        self.w_copy().start()

    def z2(self):
        at = self.at
        self.w_copy().wait_recv()
        rows, cols = self.piece(at.f * self.rows, TWO * at.za + at.zb, ONE)
        total = self.acc[rows, cols] + self.rz[ONE][...]
        rows, cols = self.piece(ZERO, TWO * at.za + at.zb, ONE)
        self.out[rows, cols] = total.astype(BF16)
        self.z_copy().start()

    def x2(self):
        self.z_copy().wait_recv()
        self.x_copy().start()

    def finish(self):
        self.x_copy().wait_recv()

    def drain_acc(self):
        for i in range(4):
            self.d_copy(i).wait_send()
            self.xy1_copy(i).wait_send()
        for i in range(TWO):
            self.xy2_copy(i).wait_send()
        self.y_copy().wait_send()
        self.w_copy().wait_send()

    def drain_out(self):
        self.z_copy().wait_send()
        self.x_copy().wait_send()

    def drain(self):
        self.drain_acc()
        self.drain_out()

class Small:

    def __init__(self, at, sm, smr, smk, smz, send, recv):
        self.at, self.sm, self.smr, self.smk, self.smz, self.send, self.recv = (at, sm, smr, smk, smz, send, recv)
        self.base = NG * NSEM

    def pair(self):
        return remote(self.sm, self.smr, self.send, self.recv, self.base, self.at.sib)

    def plane(self, j):
        v = self.smk.at[self.at.k]
        return remote(v, v, self.send, self.recv, self.base + ONE + j, (self.at.nd, self.at.nx, self.at.ny)[j])

    def stack(self, j):
        v = self.smz.at[self.at.z]
        return remote(v, v, self.send, self.recv, self.base + 4 + j, self.at.nz[j])

    def advance(self, i):
        if i == ZERO:
            self.pair().start()
        if i == ONE:
            self.pair().wait_recv()
            self.smk[self.at.k] = self.sm[...] + self.smr[...]
            for j in range(3):
                self.plane(j).start()
        if i == TWO:
            for j in range(3):
                self.plane(j).wait_recv()
            self.smz[self.at.z] = self.smk[ZERO] + self.smk[ONE] + (self.smk[TWO] + self.smk[3])
            for j in range(3):
                self.stack(j).start()

    def finish(self):
        for j in range(3):
            self.stack(j).wait_recv()
        return self.smz[ZERO] + self.smz[ONE] + (self.smz[TWO] + self.smz[3])

    def drain(self):
        self.pair().wait_send()
        for j in range(3):
            self.plane(j).wait_send()
            self.stack(j).wait_send()

def layer_kernel(x_hbm, pos_ref, seg_ref, relb_ref, ga_ref, gm_ref, wq_ref, wk_ref, wv_ref, wo_ref, wi0_ref, wi1_ref, wf_ref, go_hbm, y_hbm, small_ref, dq_ref, dk_ref, dv_ref, do_ref, di0_ref, di1_ref, df_ref, tab_s, pad_s, ga_s, gm_s, wqkv_s, wo_s, wi_s, wf_s, wqkvt_s, wot_s, wit_s, wft_s, xt_s, qkv_s, p_s, ctx_s, got_s, ut_s, zt_s, dgu_s, dh_s, dga_s, dgm_s, io_s, idx_s, *more):
    (acc, rd, r1, r2, rz, out, rq), more = ([more[i * NG:(i + ONE) * NG] for i in range(7)], more[7 * NG:])
    sm_s, smr_s, smk_s, smz_s, io_sem, out_sem, ag_own, ag_send, ag_recv, rs_send, rs_recv = more
    at = Place()
    barrier = pltpu.get_barrier_semaphore()
    peers = [at.sib, at.nx, at.ny, at.nd] + at.nz
    for dev in peers:
        pl.semaphore_signal(barrier, inc=ONE, device_id=dev, device_id_type=MESH)

    def rows_of(r):
        return pl.ds(pl.multiple_of(r * SEQ, SEQ), SEQ)

    def x_copy(r):
        return pltpu.make_async_copy(x_hbm.at[rows_of(r), :], io_s.at[rows_of(r), :], io_sem.at[ZERO, r])

    def go_copy(r):
        return pltpu.make_async_copy(go_hbm.at[rows_of(r), :], io_s.at[rows_of(r), :], io_sem.at[ONE, r])

    def y_copy(r):
        return pltpu.make_async_copy(io_s.at[rows_of(r), :], y_hbm.at[rows_of(r), :], io_sem.at[TWO, r])
    gather = Gather(at, (wq_ref, wk_ref, wv_ref, wo_ref, wi0_ref, wi1_ref, wf_ref), ((wqkv_s, ZERO), (wqkv_s, AW), (wqkv_s, TWO * AW), (wo_s, ZERO), (wi_s, ZERO), (wi_s, FF), (wf_s, ZERO)), ag_own, ag_send, ag_recv)
    for w in range(7):
        gather.load(w).start()
    for r in range(ROWS):
        x_copy(r).start()
    pl.semaphore_wait(barrier, len(peers))
    first, rest = ((ZERO, ONE, TWO), (3, 4, 5, 6))
    gather.begin(first, (TWO, ZERO, ONE, 3))
    gather.begin(rest, (ZERO, ONE, 3))
    setup_small(relb_ref, ga_ref, gm_ref, tab_s, pad_s, ga_s, gm_s)
    dgm_s[...] = jnp.zeros_like(dgm_s)
    dga_s[...] = jnp.zeros_like(dga_s)

    def prep(r):
        x_copy(r).wait()
        prep_row(r, io_s, ga_s, xt_s, ut_s)
        go_copy(r).start()
    loop(ROWS, prep)

    def prep_go(r):
        go_copy(r).wait()
        got_s[:, tok_slice(r)] = io_s[tok_slice(r), :].T
    loop(ROWS, prep_go)
    loop(ROWS, lambda r: table_row(r, pos_ref, seg_ref, tab_s, idx_s, p_s))
    gather.relay(first)
    gather.finish(first)
    wqkvt_s[...] = wqkv_s[...].T
    loop(TOK // 512, lambda r: qkv_block(r, wqkvt_s, ut_s, qkv_s))

    def fwd(r):
        attn_fwd_row(r, tab_s, idx_s, qkv_s, p_s, ctx_s)

        @pl.when(r == ZERO)
        def _():
            gather.relay1((3, 4))

        @pl.when(r == TWO)
        def _():
            gather.relay1((5,))

        @pl.when(r == 3)
        def _():
            gather.relay1((6,))
            gather.relay2((3, 4))
    loop(ROWS, fwd)
    gather.relay2((5, 6))
    gather.finish((3, 4))
    wot_s[...] = wo_s[...].T
    wit_s[ZERO:FF, :] = wi_s[:, ZERO:FF].T
    gather.finish((5, 6))
    wit_s[FF:TWO * FF, :] = wi_s[:, FF:TWO * FF].T
    wft_s[...] = wf_s[...].T
    mlp_in_row(ZERO, gm_s, wot_s, xt_s, ctx_s, ut_s, dh_s)

    def mlp_up(r):
        mlp_up_row(r, gm_s, wot_s, wit_s, wf_s, xt_s, ctx_s, got_s, ut_s, zt_s, dgu_s, dh_s)
    loop(ROWS, mlp_up)
    red = []
    for a in range(NG):
        if a in PAIRED:
            red.append(Paired(a, at, acc[a], rd[a], r1[a], r2[a], (rz[a], rq[a]), out[a], rs_send, rs_recv))
        else:
            red.append(Reduce(a, at, acc[a], rd[a], r1[a], r2[a], rz[a], out[a], rs_send, rs_recv))
    small = Small(at, sm_s, smr_s, smk_s, smz_s, rs_send, rs_recv)

    def cols(c, n=256):
        return pl.ds(pl.multiple_of(c * n, n), n)
    names = {'d': 'd_send', 'a': 'xy1', 'b': 'xy2', 'y': 'z1', 'w': 'w1', 'z': 'z2', 'x': 'x2'}

    def run_step(step, g):
        getattr(red[g], names[step])()

    def fire(name, i):
        steps = PLAN.get(f'{name}{i}', '')
        for step, g in zip(steps[::TWO], steps[ONE::TWO]):
            run_step(step, int(g))

    def fire_at(name, i, n, base=ZERO):
        for k in range(base, base + n):
            if f'{name}{k}' in PLAN:
                pl.when(i == k)(functools.partial(fire, name, k))
    for i in range(TWO):

        def dwf(c, i=i):
            part = pl.ds(pl.multiple_of(c * 512, 512), 512)
            acc[i][part, :] = mm_nt(zt_s[part, :], got_s[256 * i:256 * i + 256, :])
        loop(TWO, dwf)
        fire('wf', i)
    for g in range(4):

        def dwi(c, g=g):
            acc[TWO + g][:, cols(c)] = mm_nt(ut_s[...], dgu_s[cols(c + TWO * g), :])
            fire_at('wi', c + TWO * g, TWO, TWO * g)
        loop(TWO, dwi)

    def mlp_down(r):
        mlp_down_row(r, gm_s, wi_s, got_s, dgu_s, dh_s, dgm_s)
        fire_at('down', r, ROWS)
    loop(ROWS, mlp_down)

    def dwo(c):
        acc[6][:, cols(c)] = mm_nt(ctx_s[...], dh_s[cols(c), :])
    loop(TWO, dwo)
    fire('wo', ZERO)

    def bwd(r):
        attn_bwd_row(r, ga_s, wo_s, xt_s, ut_s, qkv_s, p_s, dh_s, dgu_s)
        fire_at('bwd', r, ROWS)
    loop(ROWS, bwd)
    for i in range(3):
        acc[7 + i][...] = mm_nt(ut_s[...], dgu_s[AW * i:AW * i + AW, :])
        fire('wqkv', i)
    for g in range(TWO):
        red[g].drain_acc()
        acc[g][...] = jnp.zeros_like(acc[g])

    def tail(r):
        bias_row(r, pos_ref, p_s, acc)
        fire_at('tail', r, ROWS)
        gain_row(r, wqkv_s, xt_s, dgu_s, dga_s)
        fire_at('gain', r, ROWS)
    loop(ROWS, tail)
    db_s = p_s.at[ZERO, ZERO]
    db_s[...] = jnp.zeros_like(db_s)
    bias_sums(acc, db_s)
    sm_s[ZERO:ONE, ZERO:256] = jnp.sum(p_s[ZERO, ZERO].T, axis=ZERO, keepdims=True)
    sm_s[ZERO:ONE, 256:512] = jnp.zeros((ONE, 256), F32)
    sm_s[ONE:TWO, :] = jnp.sum(dga_s[...].T, axis=ZERO, keepdims=True)
    sm_s[TWO:3, :] = jnp.sum(dgm_s[...].T, axis=ZERO, keepdims=True)
    sm_s[3:8, :] = jnp.zeros((5, 512), F32)
    small.advance(ZERO)
    fire('head', ZERO)

    def emit_out(r):
        out_row(r, io_s, wft_s, got_s, zt_s)
        y_copy(r).start()
        pl.when(r == ONE)(lambda: small.advance(ONE))
        fire_at('yrow', r, ROWS)
    loop(ROWS, emit_out)
    small.advance(TWO)
    finals = [(df_ref, ZERO, 256), (df_ref, 256, 256), (di0_ref, ZERO, 512), (di0_ref, 512, 512), (di1_ref, ZERO, 512), (di1_ref, 512, 512), (do_ref, ZERO, 512), (dq_ref, ZERO, AW), (dk_ref, ZERO, AW), (dv_ref, ZERO, AW)]
    finals = [pltpu.make_async_copy(out[g], dst.at[:, pl.ds(c, n)], out_sem.at[g]) for g, (dst, c, n) in enumerate(finals)]
    for g in range(NG):
        red[g].finish()
        finals[g].start()
    small_ref[...] = small.finish()
    for copy in finals:
        copy.wait()
    for r in range(ROWS):
        y_copy(r).wait()
    gather.drain(first, False)
    gather.drain(rest, True)
    for g in red[:TWO]:
        g.drain_out()
    for g in red[TWO:]:
        g.drain()
    small.drain()

def emit_kernel(y_in, small_ref, g0, g1, g2, g3, g4, g5, g6, y_out, db_ref, dga_ref, dgm_ref, o0, o1, o2, o3, o4, o5, o6, y_s, b0, b1, b2, b3, b4, b5, b6, in_sem, out_sem):
    pairs = [(y_in.at[pl.ds(r * SEQ, SEQ), :], y_s.at[pl.ds(r * SEQ, SEQ), :], y_out.at[pl.ds(r * SEQ, SEQ), :]) for r in range(ROWS)]
    pairs += list(zip((g0, g1, g2, g3, g4, g5, g6), (b0, b1, b2, b3, b4, b5, b6), (o0, o1, o2, o3, o4, o5, o6)))
    ins = [pltpu.make_async_copy(a, b, in_sem.at[i]) for i, (a, b, _) in enumerate(pairs)]
    outs = [pltpu.make_async_copy(b, c, out_sem.at[i]) for i, (_, b, c) in enumerate(pairs)]
    for copy in ins:
        copy.start()
    for h in range(HEADS):
        db_ref[h:h + ONE, :] = small_ref[ZERO:ONE, h * 32:(h + ONE) * 32]
    dga_ref[...] = small_ref[ONE:TWO, :]
    dgm_ref[...] = small_ref[TWO:3, :]
    for i in range(len(pairs)):
        ins[i].wait()
        outs[i].start()
    for copy in outs:
        copy.wait()

def local_layer(x_in, positions, segments, rel_bias, gain_attn, gain_mlp, wq, wk, wv, wo, wi0, wi1, wf, grad_out):
    vmem = pl.BlockSpec(memory_space=pltpu.VMEM)
    hbm = pl.BlockSpec(memory_space=pl.ANY)

    def bufs(shape_of, dtype):
        return [pltpu.VMEM(shape_of(r, c), dtype) for r, c in SHARD]

    def landing(a):
        r, c = SHARD[a]
        if a not in PAIRED:
            return ((3, r, 128) if r == 48 else (3, r // 4, c), (8, 128))
        return ((r, 256), (r, 128)) if r == 48 else ((r // TWO, c), (r // 4, c))
    outs = pl.pallas_call(layer_kernel, out_shape=[jax.ShapeDtypeStruct((TOK, DM), BF16), jax.ShapeDtypeStruct((8, 512), F32)] + [jax.ShapeDtypeStruct(w.shape, BF16) for w in (wq, wk, wv, wo, wi0, wi1, wf)], in_specs=[hbm] + [vmem] * 5 + [hbm] * 8, out_specs=[hbm, vmem] + [hbm] * 7, scratch_shapes=[pltpu.VMEM((8, 128), F32), pltpu.VMEM((128, 128), F32), pltpu.VMEM((DM, 128), F32), pltpu.VMEM((DM, 128), F32), pltpu.VMEM((DM, 3 * AW), BF16), pltpu.VMEM((AW, DM), BF16), pltpu.VMEM((DM, TWO * FF), BF16), pltpu.VMEM((FF, DM), BF16), pltpu.VMEM((3 * AW, DM), BF16), pltpu.VMEM((DM, AW), BF16), pltpu.VMEM((TWO * FF, DM), BF16), pltpu.VMEM((DM, FF), BF16), pltpu.VMEM((DM, TOK), BF16), pltpu.VMEM((3 * AW, TOK), BF16), pltpu.VMEM((HEADS, ROWS, SEQ, SEQ), F32), pltpu.VMEM((AW, TOK), BF16), pltpu.VMEM((DM, TOK), BF16), pltpu.VMEM((DM, TOK), BF16), pltpu.VMEM((FF, TOK), BF16), pltpu.VMEM((TWO * FF, TOK), BF16), pltpu.VMEM((DM, TOK), BF16), pltpu.VMEM((DM, 128), F32), pltpu.VMEM((DM, 128), F32), pltpu.VMEM((TOK, DM), BF16), pltpu.VMEM((ROWS, SEQ, SEQ), jnp.int32)] + bufs(lambda r, c: (8 * r, c), F32) + bufs(lambda r, c: (4, r, c), F32) + bufs(lambda r, c: (4, r // TWO, c), F32) + bufs(lambda r, c: (TWO, r // TWO, c), F32) + [pltpu.VMEM(landing(a)[ZERO], F32) for a in range(NG)] + bufs(lambda r, c: (r, c), BF16) + [pltpu.VMEM(landing(a)[ONE], F32) for a in range(NG)] + [pltpu.VMEM((8, 512), F32), pltpu.VMEM((8, 512), F32), pltpu.VMEM((4, 8, 512), F32), pltpu.VMEM((4, 8, 512), F32), pltpu.SemaphoreType.DMA((3, ROWS)), pltpu.SemaphoreType.DMA((NG,)), pltpu.SemaphoreType.DMA((7,)), pltpu.SemaphoreType.DMA((63,)), pltpu.SemaphoreType.DMA((63,)), pltpu.SemaphoreType.DMA((NG * NSEM + 7,)), pltpu.SemaphoreType.DMA((NG * NSEM + 7,))], compiler_params=pltpu.CompilerParams(vmem_limit_bytes=67043328, collective_id=ZERO, has_side_effects=True), name='layer')(x_in.reshape(TOK, DM), positions, segments, rel_bias.T, gain_attn.reshape(ONE, DM), gain_mlp.reshape(ONE, DM), wq, wk, wv, wo, wi0, wi1, wf, grad_out.reshape(TOK, DM))
    weights = (wq, wk, wv, wo, wi0, wi1, wf)
    outs = pl.pallas_call(emit_kernel, out_shape=[jax.ShapeDtypeStruct((TOK, DM), BF16), jax.ShapeDtypeStruct((HEADS, 32), F32), jax.ShapeDtypeStruct((ONE, DM), F32), jax.ShapeDtypeStruct((ONE, DM), F32)] + [jax.ShapeDtypeStruct(w.shape, BF16) for w in weights], in_specs=[hbm, vmem] + [hbm] * 7, out_specs=[hbm, vmem, vmem, vmem] + [hbm] * 7, scratch_shapes=[pltpu.VMEM((TOK, DM), BF16)] + [pltpu.VMEM(w.shape, BF16) for w in weights] + [pltpu.SemaphoreType.DMA((ROWS + 7,)), pltpu.SemaphoreType.DMA((ROWS + 7,))], name='emit')(*outs)
    y, db, dga, dgm = outs[:4]
    return (y.reshape(ROWS, SEQ, DM), db.T, dga.reshape(DM), dgm.reshape(DM)) + tuple(outs[4:])

def solution(mesh):
    row_spec = P(ROW_AXES)
    whole = P()
    part_spec = P('fsdp')
    in_specs = (row_spec, row_spec, row_spec, whole, whole, whole) + (part_spec,) * 7 + (row_spec,)
    out_specs = (row_spec, whole, whole, whole) + (part_spec,) * 7
    return jax.shard_map(local_layer, mesh=mesh, in_specs=in_specs, out_specs=out_specs, check_vma=False)
```
